256 devices in a mesh: blk: 2 (over y_lo), sector: 128 (over y_hi, z, x, core).
Axes of the slice: x: 4, y: 4 (y_hi: 2, y_lo: 2; y = y_hi * 2 + y_lo), z: 8, core: 2. Of those that a mesh axis runs over, the one named last changes fastest.
Arguments:
- state: float32 [5, 6, 6, 6, 32768], P(None, None, None, None, ('blk', 'sector')), may hold values from -6 to 6
- mean_flow: float32 [2, 4], replicated, may hold values from 0.2 to 1
- sector_offset: int32 [2], replicated, may hold values from 0 to 127
- frac_index: int32 [2], replicated, may hold values from 0 to 31
Outputs:
- new_state: float32 [5, 6, 6, 6, 32768], P(None, None, None, None, ('blk', 'sector'))
The draws below stay inside these ranges and needn't reach their ends.
All inputs are finite; a program needn't handle non-finite values.
Results may differ from the reference program's by a relative error of at most 0.0003.
Values sent between devices are 32-bit elements; how exact they have to be, the bound alone decides.
No kernel may reach another device: no remote copies, remote signals or barrier semaphores. Data moves between devices by JAX's collectives and lax.ppermute only.
A program may use at most 192 MiB of HBM per device.

```python
import math
import jax
import jax.numpy as jnp
import numpy as np
from jax import lax

VARS = 5
NODES = 6
FRACS = 4
SECTIONS = 2
EA = 8
ER = 4
EZ = 4
CELLS = 32768
N_SECTOR = 128


def steps_of(stream_key, extent, shards, low, top_value):
    loudness = 1.0
    for axis_at, shards_of in shards:
        steps = jax.random.uniform(jax.random.fold_in(jax.random.fold_in(stream_key, 6), axis_at), (shards_of,), jnp.float32, low / len(shards), top_value / len(shards))
        loudness = loudness * jnp.repeat(jnp.exp(steps), extent[axis_at] // shards_of).reshape((-1,) + (1,) * (len(extent) - 1 - axis_at))
    return loudness


def bell_draw(stream_key, shape, deviation, bound, cuts=(), kind=jnp.bfloat16):
    factor_of = steps_of(stream_key, shape, cuts, -0.22, 0.18) if cuts else 1.0
    result = jax.random.normal(stream_key, shape, jnp.float32) * deviation * factor_of
    return jnp.minimum(jnp.maximum(result, -bound), bound).astype(kind)


def setup_inputs(seed: int = 0) -> dict:
    arg_keys = jax.random.split(jax.random.key(seed), 5)
    state = bell_draw(arg_keys[0], (VARS, NODES, NODES, NODES, CELLS), 1.0, 6.0, ((4, 256),), jnp.float32)
    mean_flow = jnp.clip(jax.random.uniform(arg_keys[1], (2, 4), jnp.float32, 0.2, 1.0), 0.2, 1.0)
    sector_offset = jax.random.randint(arg_keys[2], (SECTIONS,), 0, N_SECTOR).astype(jnp.int32)
    frac_index = jax.random.randint(arg_keys[3], (SECTIONS,), 0, EA * FRACS).astype(jnp.int32)
    return {"state": state, "mean_flow": mean_flow, "sector_offset": sector_offset, "frac_index": frac_index}


HIGHEST = lax.Precision.HIGHEST
TIME_STEP = 0.02

def lobatto_points(number):
    outer = math.sqrt(1.0 / 3.0 + 2.0 * math.sqrt(7.0) / 21.0)
    inner = math.sqrt(1.0 / 3.0 - 2.0 * math.sqrt(7.0) / 21.0)
    return np.array([-1.0, -outer, -inner, inner, outer, 1.0])

def derivative_matrix(points):
    number = points.shape[0]
    barycentric = np.array([1.0 / np.prod([points[column] - points[another] for another in range(number) if another != column]) for column in range(number)])
    matrix = np.zeros((number, number))
    for target in range(number):
        for source in range(number):
            if target != source:
                matrix[target, source] = barycentric[source] / barycentric[target] / (points[target] - points[source])
        matrix[target, target] = -np.sum(matrix[target])
    return matrix

def lagrange_weights(points, where_at):
    number = points.shape[0]
    columns = []
    for source in range(number):
        weight = jnp.ones_like(where_at)
        for another in range(number):
            if another != source:
                weight = weight * (where_at - points[another]) / (points[source] - points[another])
        columns.append(weight)
    return jnp.stack(columns, axis=1)

def mortar_tables(points, fraction):
    scaled = jnp.asarray((points + 1.0) / 2.0, jnp.float32)
    stator_upper = scaled > fraction
    stator_local = jnp.where(stator_upper, scaled - fraction, scaled - fraction + 1.0) * 2.0 - 1.0
    rotor_upper = scaled + fraction >= 1.0
    rotor_local = jnp.where(rotor_upper, scaled + fraction - 1.0, scaled + fraction) * 2.0 - 1.0
    return (stator_upper, lagrange_weights(points, stator_local), rotor_upper, lagrange_weights(points, rotor_local))

def mortar_values(lower_pick, upper_pick, choose_upper, weights):
    lower_value = jnp.einsum('ts,vrsRE->vrtRE', weights, lower_pick, precision=HIGHEST)
    upper_value = jnp.einsum('ts,vrsRE->vrtRE', weights, upper_pick, precision=HIGHEST)
    return jnp.where(choose_upper[None, None, :, None, None], upper_value, lower_value)

def flux_along(quantity, flow_row, direction):
    along_speed = flow_row[direction - 1]
    sound_speed = flow_row[3]
    pieces = [along_speed * quantity[member] for member in range(quantity.shape[0])]
    pieces[0] = pieces[0] + sound_speed * quantity[direction]
    pieces[direction] = pieces[direction] + sound_speed * quantity[0]
    return jnp.stack(pieces)

def face_jump(inside, outside, flow_inside, flow_outside, direction, normal, spread):
    flux_gap = flux_along(outside, flow_outside, direction) - flux_along(inside, flow_inside, direction)
    return 0.5 * normal * flux_gap - 0.5 * spread * (outside - inside)

def interface_correction(inside, outside, flow_inside, flow_outside, normal, spread, lift_factor):
    return -lift_factor * 2.0 * face_jump(inside, outside, flow_inside, flow_outside, 3, normal, spread)

def local_rate(current, flow_row, spreads, west_faces, east_faces, interface_term, is_rotor):
    number = current.shape[1]
    points = lobatto_points(number)
    derivative_table = jnp.asarray(derivative_matrix(points), jnp.float32)
    lift_factor = number * (number - 1) / 2.0
    elements = current.shape[-1]
    slab_size = EA * ER
    element_index = jnp.arange(elements, dtype=jnp.int32)
    azimuth_slot = element_index % EA
    radial_slot = element_index // EA % ER
    axial_slot = element_index // slab_size
    radius = 1.0 + (radial_slot.astype(jnp.float32) + 0.5) / ER
    azimuth_scale = 2.0 / radius
    rate_sum = -(azimuth_scale * jnp.einsum('ij,vzrjE->vzriE', derivative_table, flux_along(current, flow_row, 1), precision=HIGHEST))
    rate_sum = rate_sum - 2.0 * jnp.einsum('ij,vzjaE->vziaE', derivative_table, flux_along(current, flow_row, 2), precision=HIGHEST)
    rate_sum = rate_sum - 2.0 * jnp.einsum('ij,vjraE->viraE', derivative_table, flux_along(current, flow_row, 3), precision=HIGHEST)
    left_face = current[:, :, :, 0, :]
    right_face = current[:, :, :, -1, :]
    edge_zero = jnp.zeros(left_face.shape[:-1] + (1,), current.dtype)
    outside_left = jnp.where(azimuth_slot == 0, jnp.repeat(west_faces, EA, axis=-1), jnp.concatenate([edge_zero, right_face[..., :-1]], axis=-1))
    outside_right = jnp.where(azimuth_slot == EA - 1, jnp.repeat(east_faces, EA, axis=-1), jnp.concatenate([left_face[..., 1:], edge_zero], axis=-1))
    rate_sum = rate_sum.at[:, :, :, 0, :].add(-lift_factor * azimuth_scale * face_jump(left_face, outside_left, flow_row, flow_row, 1, -1.0, spreads[0]))
    rate_sum = rate_sum.at[:, :, :, -1, :].add(-lift_factor * azimuth_scale * face_jump(right_face, outside_right, flow_row, flow_row, 1, 1.0, spreads[0]))
    wall_flip = jnp.asarray([1.0, 1.0, -1.0, 1.0, 1.0], current.dtype)[:, None, None, None]
    lower_face = current[:, :, 0, :, :]
    upper_face = current[:, :, -1, :, :]
    cycle_zero = jnp.zeros(lower_face.shape[:-1] + (EA,), current.dtype)
    outside_lower = jnp.where(radial_slot == 0, wall_flip * lower_face, jnp.concatenate([cycle_zero, upper_face[..., :-EA]], axis=-1))
    outside_upper = jnp.where(radial_slot == ER - 1, wall_flip * upper_face, jnp.concatenate([lower_face[..., EA:], cycle_zero], axis=-1))
    rate_sum = rate_sum.at[:, :, 0, :, :].add(-lift_factor * 2.0 * face_jump(lower_face, outside_lower, flow_row, flow_row, 2, -1.0, spreads[1]))
    rate_sum = rate_sum.at[:, :, -1, :, :].add(-lift_factor * 2.0 * face_jump(upper_face, outside_upper, flow_row, flow_row, 2, 1.0, spreads[1]))
    bottom_face = current[:, 0]
    top_face = current[:, -1]
    slab_zero = jnp.zeros(bottom_face.shape[:-1] + (slab_size,), current.dtype)
    outside_bottom = jnp.concatenate([slab_zero, top_face[..., :-slab_size]], axis=-1)
    outside_top = jnp.concatenate([bottom_face[..., slab_size:], slab_zero], axis=-1)
    bottom_term = -lift_factor * 2.0 * face_jump(bottom_face, outside_bottom, flow_row, flow_row, 3, -1.0, spreads[2])
    top_term = -lift_factor * 2.0 * face_jump(top_face, outside_top, flow_row, flow_row, 3, 1.0, spreads[2])
    rate_sum = rate_sum.at[:, 0].add(jnp.where((axial_slot == 0) & jnp.logical_not(is_rotor), 0.0, bottom_term))
    rate_sum = rate_sum.at[:, -1].add(jnp.where((axial_slot == EZ - 1) & is_rotor, 0.0, top_term))
    zero_term = jnp.zeros_like(interface_term)
    rate_sum = rate_sum.at[:, 0, :, :, :slab_size].add(jnp.where(is_rotor, zero_term, interface_term))
    rate_sum = rate_sum.at[:, -1, :, :, elements - slab_size:].add(jnp.where(is_rotor, interface_term, zero_term))
    return rate_sum

def to_cycle(traces):
    shaped = traces.reshape(N_SECTOR, VARS, NODES, NODES, ER, EA)
    return jnp.transpose(shaped, (1, 2, 3, 4, 0, 5)).reshape(VARS, NODES, NODES, ER, N_SECTOR * EA)

def from_cycle(traces):
    shaped = traces.reshape(VARS, NODES, NODES, ER, N_SECTOR, EA)
    return jnp.transpose(shaped, (4, 0, 1, 2, 3, 5)).reshape(N_SECTOR, VARS, NODES, NODES, ER * EA)

def reference(state, mean_flow, sector_offset, frac_index):
    elements = EA * ER * EZ
    slab_size = EA * ER
    points = lobatto_points(NODES)
    lift_factor = NODES * (NODES - 1) / 2.0
    spreads = lax.optimization_barrier(jnp.max(jnp.abs(mean_flow[:, :3]), axis=0)) + jnp.max(mean_flow[:, 3])
    row_ids = jnp.repeat(jnp.arange(2, dtype=jnp.int32), N_SECTOR)

    def section_rate(current, section_index):
        blocks = jnp.moveaxis(current.reshape(VARS, NODES, NODES, NODES, 2, N_SECTOR, elements), (4, 5), (0, 1))
        right_edge = blocks[:, :, :, :, :, -1, EA - 1::EA]
        left_edge = blocks[:, :, :, :, :, 0, 0::EA]
        west_all = jnp.roll(right_edge, 1, axis=1)
        east_all = jnp.roll(left_edge, -1, axis=1)
        rotor_cycle = to_cycle(blocks[0, :, :, -1, :, :, elements - slab_size:])
        stator_cycle = to_cycle(blocks[1, :, :, 0, :, :, :slab_size])
        whole_steps = frac_index[section_index] // FRACS
        fraction = (frac_index[section_index] % FRACS).astype(jnp.float32) / FRACS
        shift_total = sector_offset[section_index] * EA + whole_steps
        stator_upper, stator_weights, rotor_upper, rotor_weights = mortar_tables(points, fraction)
        stator_plus = mortar_values(jnp.roll(rotor_cycle, shift_total + 1, axis=4), jnp.roll(rotor_cycle, shift_total, axis=4), stator_upper, stator_weights)
        stator_term = interface_correction(stator_cycle, stator_plus, mean_flow[1], mean_flow[0], -1.0, spreads[2], lift_factor)
        rotor_plus = mortar_values(jnp.roll(stator_cycle, -shift_total, axis=4), jnp.roll(stator_cycle, -shift_total - 1, axis=4), rotor_upper, rotor_weights)
        rotor_term = interface_correction(rotor_cycle, rotor_plus, mean_flow[0], mean_flow[1], 1.0, spreads[2], lift_factor)
        interface_all = jnp.stack([from_cycle(rotor_term), from_cycle(stator_term)])

        def block_rate(packed):
            block_state, west_faces, east_faces, interface_term, row_id = packed
            return local_rate(block_state, mean_flow[row_id], spreads, west_faces, east_faces, interface_term, row_id == 0)
        rates = lax.map(block_rate, (blocks.reshape((2 * N_SECTOR,) + blocks.shape[2:]), west_all.reshape((2 * N_SECTOR,) + west_all.shape[2:]), east_all.reshape((2 * N_SECTOR,) + east_all.shape[2:]), interface_all.reshape((2 * N_SECTOR,) + interface_all.shape[2:]), row_ids))
        rates = rates.reshape((2, N_SECTOR) + rates.shape[1:])
        return jnp.moveaxis(rates, (0, 1), (4, 5)).reshape(current.shape)
    middle = state + TIME_STEP * section_rate(state, 0)
    return 0.5 * state + 0.5 * (middle + TIME_STEP * section_rate(middle, 1))
```

```python
import functools
import math

import jax
import jax.numpy as jnp
import numpy as np
from jax import lax
from jax.experimental import pallas as pl
from jax.experimental.pallas import tpu as pltpu
from jax.sharding import PartitionSpec as P

FRACS = 4
EA = 8
ER = 4
EZ = 4
VARS = 5
NODES = 6
LANES = EA * ER * EZ
SLAB = EA * ER
AXES = ("blk", "sector")
TIME_STEP = 0.02
LIFT = NODES * (NODES - 1) / 2.0
HIGH = 16
LOW = 8
FACE_TILES = 4
TRACE_TILES = 8


def lobatto_points():
    outer = math.sqrt(1.0 / 3.0 + 2.0 * math.sqrt(7.0) / 21.0)
    inner = math.sqrt(1.0 / 3.0 - 2.0 * math.sqrt(7.0) / 21.0)
    return np.array([-1.0, -outer, -inner, inner, outer, 1.0])


def derivative_matrix(points):
    number = points.shape[0]
    bary = [
        1.0 / np.prod([points[i] - points[j] for j in range(number) if j != i])
        for i in range(number)
    ]
    matrix = np.zeros((number, number))
    for i in range(number):
        for j in range(number):
            if i != j:
                matrix[i, j] = bary[j] / bary[i] / (points[i] - points[j])
        matrix[i, i] = -np.sum(matrix[i])
    return matrix


POINTS = lobatto_points()
DERIV = derivative_matrix(POINTS).astype(np.float32)


def iota(axis):
    return lax.broadcasted_iota(jnp.int32, (NODES, LANES), axis)


def by_row(values):
    row = iota(0)
    result = jnp.full((NODES, LANES), float(values[0]), jnp.float32)
    for at in range(1, NODES):
        result = jnp.where(row == at, float(values[at]), result)
    return result


def azimuth_scale():
    radial = lax.shift_right_logical(iota(1), 3) & (ER - 1)
    result = jnp.full((NODES, LANES), 2.0 / (1.0 + 0.5 / ER), jnp.float32)
    for at in range(1, ER):
        result = jnp.where(radial == at, 2.0 / (1.0 + (at + 0.5) / ER), result)
    return result


def spread(flow, direction):
    return jnp.maximum(
        jnp.abs(flow[0, direction - 1]), jnp.abs(flow[1, direction - 1])
    ) + jnp.maximum(flow[0, 3], flow[1, 3])


def turned(tile, by):
    by = by % LANES
    return pltpu.roll(tile, by, 1) if by else tile


def jump_rates(jumps, direction, normal, speed, sound, wide, factor):
    along = -factor * 0.5 * (normal * speed - wide)
    across = -factor * 0.5 * normal * sound
    rates = [along * jump for jump in jumps]
    rates[0] = rates[0] + across * jumps[direction]
    rates[direction] = rates[direction] + across * jumps[0]
    return rates


def volume_kernel(flow, *refs, second):
    if second:
        start, x, out = refs
    else:
        x, out = refs
    gain = TIME_STEP * (0.5 if second else 1.0)
    row = lax.axis_index("blk")
    rotor = (row == 0).astype(jnp.float32)
    speed = [flow[row, at] for at in range(3)]
    sound = flow[row, 3]
    wide = [spread(flow, at + 1) for at in range(3)]
    lane = iota(1)
    slot = lane & (EA - 1)
    radial = lax.shift_right_logical(lane, 3) & (ER - 1)
    layer = lax.shift_right_logical(lane, 5)
    scale = azimuth_scale()
    columns = [scale * by_row(DERIV[:, at]) for at in range(NODES)]
    c_axial, c_radial, c_azimuth = -gain * 2.0 * speed[2], -gain * 2.0 * speed[1], -gain * speed[0]
    c_sound, c_sound2 = -gain * sound, -gain * 2.0 * sound
    lift = gain * LIFT * 2.0
    for i in range(NODES):
        for b in range(NODES):
            rates = [None] * VARS
            grads = []
            for v in range(VARS):
                ga = DERIV[i, 0] * x[v, 0, b]
                gb = DERIV[b, 0] * x[v, i, 0]
                gc = columns[0] * x[v, i, b, 0:1, :]
                for j in range(1, NODES):
                    ga = ga + DERIV[i, j] * x[v, j, b]
                    gb = gb + DERIV[b, j] * x[v, i, j]
                    gc = gc + columns[j] * x[v, i, b, j : j + 1, :]
                rates[v] = c_axial * ga + c_radial * gb + c_azimuth * gc
                if v == 0:
                    grads = [gc, gb, ga]
                elif v == 1:
                    rates[0] = rates[0] + c_sound * gc
                    rates[1] = rates[1] + c_sound * grads[0]
                elif v == 2:
                    rates[0] = rates[0] + c_sound2 * gb
                    rates[2] = rates[2] + c_sound2 * grads[1]
                elif v == 3:
                    rates[0] = rates[0] + c_sound2 * ga
                    rates[3] = rates[3] + c_sound2 * grads[2]
            if b == 0 or b == NODES - 1:
                normal, by, wall = (-1.0, EA, 0) if b == 0 else (1.0, -EA, ER - 1)
                jumps = []
                for v in range(VARS):
                    inside = x[v, i, b]
                    gap = turned(x[v, i, NODES - 1 - b], by) - inside
                    at_wall = -2.0 * inside if v == 2 else jnp.zeros_like(inside)
                    jumps.append(jnp.where(radial == wall, at_wall, gap))
                terms = jump_rates(jumps, 2, normal, speed[1], sound, wide[1], lift)
                rates = [rate + term for rate, term in zip(rates, terms)]
            if i == 0 or i == NODES - 1:
                normal, by, end = (-1.0, SLAB, 0) if i == 0 else (1.0, -SLAB, EZ - 1)
                keep = rotor if i == 0 else 1.0 - rotor
                jumps = []
                for v in range(VARS):
                    inside = x[v, i, b]
                    gap = turned(x[v, NODES - 1 - i, b], by) - inside
                    jumps.append(jnp.where(layer == end, -keep * inside, gap))
                terms = jump_rates(jumps, 3, normal, speed[2], sound, wide[2], lift)
                rates = [rate + term for rate, term in zip(rates, terms)]
            for v in range(VARS):
                base = x[v, i, b]
                if second:
                    base = 0.5 * (start[v, i, b] + base)
                out[v, i, b] = base + rates[v]
        left = [x[v, i, :, 0, :] for v in range(VARS)]
        right = [x[v, i, :, NODES - 1, :] for v in range(VARS)]
        lower = [
            jnp.where(slot == 0, 0.0, turned(right[v], 1) - left[v]) for v in range(VARS)
        ]
        upper = [
            jnp.where(slot == EA - 1, 0.0, turned(left[v], -1) - right[v]) for v in range(VARS)
        ]
        factor = gain * LIFT * scale
        lower = jump_rates(lower, 1, -1.0, speed[0], sound, wide[0], factor)
        upper = jump_rates(upper, 1, 1.0, speed[0], sound, wide[0], factor)
        for v in range(VARS):
            out[v, i, :, 0, :] = out[v, i, :, 0, :] + lower[v]
            out[v, i, :, NODES - 1, :] = out[v, i, :, NODES - 1, :] + upper[v]


def pack(x, west, east):
    slot = iota(1) & (EA - 1)
    group = lax.shift_right_logical(iota(1), 5)
    zeros = jnp.zeros((NODES, LANES), jnp.float32)
    for p in range(FACE_TILES):
        low, high = zeros, zeros
        for o in range(EA):
            t = p * EA + o
            if t < VARS * NODES:
                v, a = t // NODES, t % NODES
                low = jnp.where(slot == o, turned(x[v, a, :, 0, :], o), low)
                high = jnp.where(slot == o, turned(x[v, a, :, NODES - 1, :], o - EA + 1), high)
        west[p] = low
        east[p] = high

    def trace(plane, start):
        for p in range(TRACE_TILES):
            tile = zeros
            for o in range(EZ):
                t = p * EZ + o
                if t < VARS * NODES:
                    v, b = t // NODES, t % NODES
                    tile = jnp.where(group == o, turned(x[v, plane, b], SLAB * o - start), tile)
            west[FACE_TILES + p] = tile

    is_rotor = lax.axis_index("blk") == 0

    @pl.when(is_rotor)
    def _():
        trace(NODES - 1, LANES - SLAB)

    @pl.when(jnp.logical_not(is_rotor))
    def _():
        trace(0, 0)


def pack_kernel(x, west, east):
    pack(x, west, east)


def mortar_kernel(frac, own, beyond, out, *, section):
    is_rotor = lax.axis_index("blk") == 0
    index = frac[section]
    whole = index // FRACS
    part = (index % FRACS).astype(jnp.float32) * (1.0 / FRACS)
    first = jnp.where(is_rotor, EA - 1 - whole, whole)
    scaled = by_row((POINTS + 1.0) / 2.0)
    for_stator = scaled - part
    for_rotor = scaled + part
    at = jnp.where(is_rotor, for_stator, for_rotor)
    upper = jnp.where(
        is_rotor, (scaled > part).astype(jnp.int32), (for_rotor >= 1.0).astype(jnp.int32)
    )
    step = jnp.where(is_rotor, 1 - upper, -upper).astype(jnp.float32)
    is_upper = upper == 1
    local = (at + step) * 2.0 - 1.0
    weights = []
    for s in range(NODES):
        weight = jnp.ones((NODES, LANES), jnp.float32)
        for j in range(NODES):
            if j != s:
                weight = weight * ((local - float(POINTS[j])) * float(1.0 / (POINTS[s] - POINTS[j])))
        weights.append(weight)
    slot = iota(1) & (EA - 1)

    def window(mine, theirs, begin):
        return jnp.where(
            slot + begin < EA,
            pltpu.roll(mine, (LANES - begin) & (LANES - 1), 1),
            pltpu.roll(theirs, (LANES + EA - begin) & (LANES - 1), 1),
        )

    for p in range(TRACE_TILES):
        mine, theirs = own[FACE_TILES + p], beyond[FACE_TILES + p]
        low = window(mine, theirs, first)
        high = window(mine, theirs, first + 1)
        total = None
        for s in range(NODES):
            pick = jnp.where(
                is_upper,
                jnp.broadcast_to(high[s : s + 1, :], (NODES, LANES)),
                jnp.broadcast_to(low[s : s + 1, :], (NODES, LANES)),
            )
            total = weights[s] * pick if total is None else total + weights[s] * pick
        out[p] = total


def close_kernel(flow, acc, x, from_west, from_east, plus, out, *messages, second):
    gain = TIME_STEP * (0.5 if second else 1.0)
    row = lax.axis_index("blk")
    is_rotor = row == 0
    speed = [flow[row, at] for at in range(3)]
    sound = flow[row, 3]
    far_speed, far_sound = flow[1 - row, 2], flow[1 - row, 3]
    wide = [spread(flow, at + 1) for at in range(3)]
    lane = iota(1)
    slot = lane & (EA - 1)
    layer = lax.shift_right_logical(lane, 5)
    factor = gain * LIFT * azimuth_scale()
    for i in range(NODES):
        for v in range(VARS):
            out[v, i] = acc[v, i]
        lower, upper = [], []
        for v in range(VARS):
            p, o = divmod(v * NODES + i, EA)
            gap = turned(from_west[p], -o) - x[v, i, :, 0, :]
            lower.append(jnp.where(slot == 0, gap, 0.0))
            gap = turned(from_east[p], EA - 1 - o) - x[v, i, :, NODES - 1, :]
            upper.append(jnp.where(slot == EA - 1, gap, 0.0))
        lower = jump_rates(lower, 1, -1.0, speed[0], sound, wide[0], factor)
        upper = jump_rates(upper, 1, 1.0, speed[0], sound, wide[0], factor)
        for v in range(VARS):
            out[v, i, :, 0, :] = out[v, i, :, 0, :] + lower[v]
            out[v, i, :, NODES - 1, :] = out[v, i, :, NODES - 1, :] + upper[v]

    def interface(plane, start, normal):
        scale = -gain * LIFT * 2.0
        mine = scale * 0.5 * (wide[2] - normal * speed[2])
        theirs = scale * 0.5 * (normal * far_speed - wide[2])
        cross_mine = -scale * 0.5 * normal * sound
        cross_theirs = scale * 0.5 * normal * far_sound
        for b in range(NODES):
            inside = [x[v, plane, b] for v in range(VARS)]
            outside = []
            for v in range(VARS):
                p, o = divmod(v * NODES + b, EZ)
                outside.append(turned(plus[p], start - SLAB * o))
            for v in range(VARS):
                term = mine * inside[v] + theirs * outside[v]
                if v == 0 or v == 3:
                    term = term + (cross_mine * inside[3 - v] + cross_theirs * outside[3 - v])
                out[v, plane, b] = out[v, plane, b] + jnp.where(layer == start // SLAB, term, 0.0)

    @pl.when(is_rotor)
    def _():
        interface(NODES - 1, LANES - SLAB, 1.0)

    @pl.when(jnp.logical_not(is_rotor))
    def _():
        interface(0, 0, -1.0)

    if messages:
        pack(out, *messages)


VMEM = pl.BlockSpec(memory_space=pltpu.VMEM)
SMEM = pl.BlockSpec(memory_space=pltpu.SMEM)
BLOCK = jax.ShapeDtypeStruct((VARS, NODES, NODES, NODES, LANES), jnp.float32)
TO_WEST = jax.ShapeDtypeStruct((FACE_TILES + TRACE_TILES, NODES, LANES), jnp.float32)
TO_EAST = jax.ShapeDtypeStruct((FACE_TILES, NODES, LANES), jnp.float32)
TRACE = jax.ShapeDtypeStruct((TRACE_TILES, NODES, LANES), jnp.float32)


def call(body, specs, out_shape, name, flops=1000):
    several = isinstance(out_shape, tuple)
    return pl.pallas_call(
        body,
        in_specs=specs,
        out_specs=(VMEM,) * len(out_shape) if several else VMEM,
        out_shape=out_shape,
        cost_estimate=pl.CostEstimate(flops=flops, transcendentals=0, bytes_accessed=10**6),
        name=name,
    )


def rotated(message, offset, count):
    high = offset // LOW
    low = offset % LOW

    def far(turn):
        shift = LOW * turn
        pairs = [(i, count + (i + shift + 1) % count) for i in range(count)]
        pairs += [(count + i, (i - shift) % count) for i in range(count)]
        return lambda array: lax.ppermute(array, AXES, pairs)

    def near(turn):
        pairs = [(i, (i - turn) % count) for i in range(count)]
        pairs += [(count + i, count + (i + turn) % count) for i in range(count)]
        if turn == 0:
            return lambda array: array
        return lambda array: lax.ppermute(array, AXES, pairs)

    message = lax.switch(high, [far(at) for at in range(count // LOW)], message)
    return lax.switch(low, [near(at) for at in range(LOW)], message)


def per_device(state, mean_flow, sector_offset, frac_index):
    count = lax.axis_size("sector")
    up = [(i, (i + 1) % count) for i in range(count)]
    down = [(j, i) for i, j in up]
    start = state
    current = state
    west, east = call(pack_kernel, [VMEM], (TO_WEST, TO_EAST), "pack")(state)
    for section in range(2):
        second = section == 1
        from_east = lax.ppermute(west, "sector", down)
        from_west = lax.ppermute(east, "sector", up)
        inputs = (start, current) if second else (current,)
        partial = call(
            functools.partial(volume_kernel, second=second),
            [SMEM] + [VMEM] * len(inputs),
            BLOCK,
            "volume",
            flops=10**8,
        )(mean_flow, *inputs)
        message = call(
            functools.partial(mortar_kernel, section=section), [SMEM, VMEM, VMEM], TRACE, "mortar"
        )(frac_index, west, from_east)
        plus = rotated(message, sector_offset[section], count)
        shapes = (BLOCK,) if second else (BLOCK, TO_WEST, TO_EAST)
        results = call(
            functools.partial(close_kernel, second=second),
            [SMEM] + [VMEM] * 5,
            shapes,
            "close",
        )(mean_flow, partial, current, from_west, from_east, plus)
        current = results[0]
        if not second:
            west, east = results[1:]
    return current


def solution(mesh):
    in_specs = (P(None, None, None, None, ("blk", "sector")), P(), P(), P())
    out_specs = P(None, None, None, None, ("blk", "sector"))
    return jax.shard_map(
        per_device, mesh=mesh, in_specs=in_specs, out_specs=out_specs, check_vma=False
    )
```

```python
import functools
import math

import jax
import jax.numpy as jnp
import numpy as np
from jax import lax
from jax.experimental import pallas as pl
from jax.experimental.pallas import tpu as pltpu
from jax.sharding import PartitionSpec as P

FRACS = 4
EA = 8
ER = 4
EZ = 4
VARS = 5
NODES = 6
LANES = EA * ER * EZ
SLAB = EA * ER
AXES = ("blk", "sector")
TIME_STEP = 0.02
LIFT = NODES * (NODES - 1) / 2.0
HIGH = 16
LOW = 8
FACE_TILES = VARS
TRACE_TILES = 8


def lobatto_points():
    outer = math.sqrt(1.0 / 3.0 + 2.0 * math.sqrt(7.0) / 21.0)
    inner = math.sqrt(1.0 / 3.0 - 2.0 * math.sqrt(7.0) / 21.0)
    return np.array([-1.0, -outer, -inner, inner, outer, 1.0])


def derivative_matrix(points):
    number = points.shape[0]
    bary = [
        1.0 / np.prod([points[i] - points[j] for j in range(number) if j != i])
        for i in range(number)
    ]
    matrix = np.zeros((number, number))
    for i in range(number):
        for j in range(number):
            if i != j:
                matrix[i, j] = bary[j] / bary[i] / (points[i] - points[j])
        matrix[i, i] = -np.sum(matrix[i])
    return matrix


POINTS = lobatto_points()
DERIV = derivative_matrix(POINTS).astype(np.float32)


def iota(axis):
    return lax.broadcasted_iota(jnp.int32, (NODES, LANES), axis)


def by_row(values):
    row = iota(0)
    result = jnp.full((NODES, LANES), float(values[0]), jnp.float32)
    for at in range(1, NODES):
        result = jnp.where(row == at, float(values[at]), result)
    return result


def azimuth_scale():
    radial = lax.shift_right_logical(iota(1), 3) & (ER - 1)
    result = jnp.full((NODES, LANES), 2.0 / (1.0 + 0.5 / ER), jnp.float32)
    for at in range(1, ER):
        result = jnp.where(radial == at, 2.0 / (1.0 + (at + 0.5) / ER), result)
    return result


def spread(flow, direction):
    return jnp.maximum(
        jnp.abs(flow[0, direction - 1]), jnp.abs(flow[1, direction - 1])
    ) + jnp.maximum(flow[0, 3], flow[1, 3])


def turned(tile, by):
    by = by % LANES
    return pltpu.roll(tile, by, 1) if by else tile


def jump_rates(jumps, direction, normal, speed, sound, wide, factor):
    along = -factor * 0.5 * (normal * speed - wide)
    across = -factor * 0.5 * normal * sound
    rates = [along * jump for jump in jumps]
    rates[0] = rates[0] + across * jumps[direction]
    rates[direction] = rates[direction] + across * jumps[0]
    return rates


def coefficient(index, column):
    value = jnp.float32(DERIV[0, column])
    for at in range(1, NODES):
        value = jnp.where(index == at, jnp.float32(DERIV[at, column]), value)
    return value


def volume_kernel(flow, *refs, second):
    if second:
        start, x, out = refs
    else:
        x, out = refs
    gain = TIME_STEP * (0.5 if second else 1.0)
    row = lax.axis_index("blk")
    rotor = (row == 0).astype(jnp.float32)
    speed = [flow[row, at] for at in range(3)]
    sound = flow[row, 3]
    wide = [spread(flow, at + 1) for at in range(3)]
    lane = iota(1)
    slot = lane & (EA - 1)
    radial = lax.shift_right_logical(lane, 3) & (ER - 1)
    layer = lax.shift_right_logical(lane, 5)
    scale = azimuth_scale()
    columns = [scale * by_row(DERIV[:, at]) for at in range(NODES)]
    c_axial, c_radial, c_azimuth = -gain * 2.0 * speed[2], -gain * 2.0 * speed[1], -gain * speed[0]
    c_sound, c_sound2 = -gain * sound, -gain * 2.0 * sound
    lift = gain * LIFT * 2.0

    def at_layer(i, carry):
        axial = [coefficient(i, j) for j in range(NODES)]
        for b in range(NODES):
            rates = [None] * VARS
            grads = []
            for v in range(VARS):
                ga = axial[0] * x[v, 0, b]
                gb = DERIV[b, 0] * x[v, i, 0]
                gc = columns[0] * x[v, i, b, 0:1, :]
                for j in range(1, NODES):
                    ga = ga + axial[j] * x[v, j, b]
                    gb = gb + DERIV[b, j] * x[v, i, j]
                    gc = gc + columns[j] * x[v, i, b, j : j + 1, :]
                rates[v] = c_axial * ga + c_radial * gb + c_azimuth * gc
                if v == 0:
                    grads = [gc, gb, ga]
                elif v == 1:
                    rates[0] = rates[0] + c_sound * gc
                    rates[1] = rates[1] + c_sound * grads[0]
                elif v == 2:
                    rates[0] = rates[0] + c_sound2 * gb
                    rates[2] = rates[2] + c_sound2 * grads[1]
                elif v == 3:
                    rates[0] = rates[0] + c_sound2 * ga
                    rates[3] = rates[3] + c_sound2 * grads[2]
            if b == 0 or b == NODES - 1:
                normal, by, wall = (-1.0, EA, 0) if b == 0 else (1.0, -EA, ER - 1)
                jumps = []
                for v in range(VARS):
                    inside = x[v, i, b]
                    gap = turned(x[v, i, NODES - 1 - b], by) - inside
                    at_wall = -2.0 * inside if v == 2 else jnp.zeros_like(inside)
                    jumps.append(jnp.where(radial == wall, at_wall, gap))
                terms = jump_rates(jumps, 2, normal, speed[1], sound, wide[1], lift)
                rates = [rate + term for rate, term in zip(rates, terms)]
            for v in range(VARS):
                base = x[v, i, b]
                if second:
                    base = 0.5 * (start[v, i, b] + base)
                out[v, i, b] = base + rates[v]
        left = [x[v, i, :, 0, :] for v in range(VARS)]
        right = [x[v, i, :, NODES - 1, :] for v in range(VARS)]
        lower = [
            jnp.where(slot == 0, 0.0, turned(right[v], 1) - left[v]) for v in range(VARS)
        ]
        upper = [
            jnp.where(slot == EA - 1, 0.0, turned(left[v], -1) - right[v]) for v in range(VARS)
        ]
        factor = gain * LIFT * scale
        lower = jump_rates(lower, 1, -1.0, speed[0], sound, wide[0], factor)
        upper = jump_rates(upper, 1, 1.0, speed[0], sound, wide[0], factor)
        for v in range(VARS):
            out[v, i, :, 0, :] = out[v, i, :, 0, :] + lower[v]
            out[v, i, :, NODES - 1, :] = out[v, i, :, NODES - 1, :] + upper[v]
        return carry

    lax.fori_loop(0, NODES, at_layer, 0)

    def at_radial(b, carry):
        for i in (0, NODES - 1):
            normal, by, end = (-1.0, SLAB, 0) if i == 0 else (1.0, -SLAB, EZ - 1)
            keep = rotor if i == 0 else 1.0 - rotor
            jumps = []
            for v in range(VARS):
                inside = x[v, i, b]
                gap = turned(x[v, NODES - 1 - i, b], by) - inside
                jumps.append(jnp.where(layer == end, -keep * inside, gap))
            terms = jump_rates(jumps, 3, normal, speed[2], sound, wide[2], lift)
            for v in range(VARS):
                out[v, i, b] = out[v, i, b] + terms[v]
        return carry

    lax.fori_loop(0, NODES, at_radial, 0)


def pack(x, first, other):
    is_rotor = lax.axis_index("blk") == 0
    slot = iota(1) & (EA - 1)
    group = lax.shift_right_logical(iota(1), 5)
    zeros = jnp.zeros((NODES, LANES), jnp.float32)
    for v in range(VARS):
        low, high = zeros, zeros
        for a in range(NODES):
            low = jnp.where(slot == a, turned(x[v, a, :, 0, :], a), low)
            high = jnp.where(slot == a, turned(x[v, a, :, NODES - 1, :], a - EA + 1), high)
        first[v, 0:NODES, :] = jnp.where(is_rotor, high, low)
        other[v, 0:NODES, :] = jnp.where(is_rotor, low, high)

    def trace(plane, start):
        for p in range(TRACE_TILES):
            tile = zeros
            for o in range(EZ):
                t = p * EZ + o
                if t < VARS * NODES:
                    v, b = t // NODES, t % NODES
                    tile = jnp.where(group == o, turned(x[v, plane, b], SLAB * o - start), tile)
            first[FACE_TILES + p, 0:NODES, :] = tile

    @pl.when(is_rotor)
    def _():
        trace(NODES - 1, LANES - SLAB)

    @pl.when(jnp.logical_not(is_rotor))
    def _():
        trace(0, 0)


def pack_kernel(x, first, other):
    pack(x, first, other)


def mortar_kernel(frac, own, beyond, out, *, section):
    is_rotor = lax.axis_index("blk") == 0
    index = frac[section]
    whole = lax.shift_right_logical(index, 2)
    part = (index & (FRACS - 1)).astype(jnp.float32) * (1.0 / FRACS)
    begin = jnp.where(is_rotor, EA - 1 - whole, whole)
    scaled = by_row((POINTS + 1.0) / 2.0)
    for_stator = scaled - part
    for_rotor = scaled + part
    at = jnp.where(is_rotor, for_stator, for_rotor)
    upper = jnp.where(
        is_rotor, (scaled > part).astype(jnp.int32), (for_rotor >= 1.0).astype(jnp.int32)
    )
    step = jnp.where(is_rotor, 1 - upper, -upper).astype(jnp.float32)
    is_upper = upper == 1
    local = (at + step) * 2.0 - 1.0
    weights = []
    for s in range(NODES):
        weight = jnp.ones((NODES, LANES), jnp.float32)
        for j in range(NODES):
            if j != s:
                weight = weight * ((local - float(POINTS[j])) * float(1.0 / (POINTS[s] - POINTS[j])))
        weights.append(weight)
    slot = iota(1) & (EA - 1)

    def window(lead, trail, begin):
        return jnp.where(
            slot + begin < EA,
            pltpu.roll(lead, (LANES - begin) & (LANES - 1), 1),
            pltpu.roll(trail, (LANES + EA - begin) & (LANES - 1), 1),
        )

    for p in range(TRACE_TILES):
        mine = own[FACE_TILES + p, 0:NODES, :]
        theirs = beyond[FACE_TILES + p, 0:NODES, :]
        lead = jnp.where(is_rotor, theirs, mine)
        trail = jnp.where(is_rotor, mine, theirs)
        low = window(lead, trail, begin)
        high = window(lead, trail, begin + 1)
        total = None
        for s in range(NODES):
            pick = jnp.where(
                is_upper,
                jnp.broadcast_to(high[s : s + 1, :], (NODES, LANES)),
                jnp.broadcast_to(low[s : s + 1, :], (NODES, LANES)),
            )
            total = weights[s] * pick if total is None else total + weights[s] * pick
        out[p, 0:NODES, :] = total


def close_kernel(flow, acc, x, first, other, plus, out, *messages, second):
    gain = TIME_STEP * (0.5 if second else 1.0)
    row = lax.axis_index("blk")
    is_rotor = row == 0
    speed = [flow[row, at] for at in range(3)]
    sound = flow[row, 3]
    far_speed, far_sound = flow[1 - row, 2], flow[1 - row, 3]
    wide = [spread(flow, at + 1) for at in range(3)]
    lane = iota(1)
    slot = lane & (EA - 1)
    layer = lax.shift_right_logical(lane, 5)
    factor = gain * LIFT * azimuth_scale()

    def at_layer(i, carry):
        for v in range(VARS):
            out[v, i] = acc[v, i]
        lower, upper = [], []
        for v in range(VARS):
            one, two = first[v, 0:NODES, :], other[v, 0:NODES, :]
            west = jnp.where(is_rotor, one, two)
            east = jnp.where(is_rotor, two, one)
            gap = pltpu.roll(west, (LANES - i) & (LANES - 1), 1) - x[v, i, :, 0, :]
            lower.append(jnp.where(slot == 0, gap, 0.0))
            gap = pltpu.roll(east, EA - 1 - i, 1) - x[v, i, :, NODES - 1, :]
            upper.append(jnp.where(slot == EA - 1, gap, 0.0))
        lower = jump_rates(lower, 1, -1.0, speed[0], sound, wide[0], factor)
        upper = jump_rates(upper, 1, 1.0, speed[0], sound, wide[0], factor)
        for v in range(VARS):
            out[v, i, :, 0, :] = out[v, i, :, 0, :] + lower[v]
            out[v, i, :, NODES - 1, :] = out[v, i, :, NODES - 1, :] + upper[v]
        return carry

    lax.fori_loop(0, NODES, at_layer, 0)

    def interface(plane, start, normal):
        scale = -gain * LIFT * 2.0
        mine = scale * 0.5 * (wide[2] - normal * speed[2])
        theirs = scale * 0.5 * (normal * far_speed - wide[2])
        cross_mine = -scale * 0.5 * normal * sound
        cross_theirs = scale * 0.5 * normal * far_sound
        for b in range(NODES):
            inside = [x[v, plane, b] for v in range(VARS)]
            outside = []
            for v in range(VARS):
                p, o = divmod(v * NODES + b, EZ)
                outside.append(turned(plus[p, 0:NODES, :], start - SLAB * o))
            for v in range(VARS):
                term = mine * inside[v] + theirs * outside[v]
                if v == 0 or v == 3:
                    term = term + (cross_mine * inside[3 - v] + cross_theirs * outside[3 - v])
                out[v, plane, b] = out[v, plane, b] + jnp.where(layer == start // SLAB, term, 0.0)

    @pl.when(is_rotor)
    def _():
        interface(NODES - 1, LANES - SLAB, 1.0)

    @pl.when(jnp.logical_not(is_rotor))
    def _():
        interface(0, 0, -1.0)

    if messages:
        pack(out, *messages)


VMEM = pl.BlockSpec(memory_space=pltpu.VMEM)
SMEM = pl.BlockSpec(memory_space=pltpu.SMEM)
BLOCK = (VARS, NODES, NODES, NODES, LANES)
FIRST = (FACE_TILES + TRACE_TILES, 8, LANES)
OTHER = (FACE_TILES, 8, LANES)
TRACE = (TRACE_TILES, 8, LANES)


def call(body, scalars, arrays, shapes, name, flops=1000, keep=True):
    make = pltpu.VMEM if keep else jax.ShapeDtypeStruct
    arrays = [pltpu.with_memory_space_constraint(array, pltpu.VMEM) for array in arrays]
    results = pl.pallas_call(
        body,
        in_specs=[SMEM] * len(scalars) + [VMEM] * len(arrays),
        out_specs=tuple(VMEM for _ in shapes),
        out_shape=tuple(make(shape, jnp.float32) for shape in shapes),
        cost_estimate=pl.CostEstimate(flops=flops, transcendentals=0, bytes_accessed=10**6),
        compiler_params=pltpu.CompilerParams(vmem_limit_bytes=16 * 2**20),
        name=name,
    )(*scalars, *arrays)
    return results if len(shapes) > 1 else results[0]


def rotated(message, offset, count):
    high = lax.shift_right_logical(offset, 3)
    low = offset & (LOW - 1)

    def far(turn):
        shift = LOW * turn
        pairs = [(i, count + (i + shift) % count) for i in range(count)]
        pairs += [(count + (i + shift) % count, i) for i in range(count)]
        return lambda array: lax.ppermute(array, AXES, pairs)

    def near(turn):
        if turn == 0:
            return lambda array: array
        pairs = [(i, (i - turn) % count) for i in range(count)]
        pairs += [(count + i, count + (i + turn) % count) for i in range(count)]
        return lambda array: lax.ppermute(array, AXES, pairs)

    message = lax.switch(high, [far(at) for at in range(count // LOW)], message)
    return lax.switch(low, [near(at) for at in range(LOW)], message)


def per_device(state, mean_flow, sector_offset, frac_index):
    count = lax.axis_size("sector")
    ahead = [(i, (i + 1) % count) for i in range(count)]
    ahead += [(count + (i + 1) % count, count + i) for i in range(count)]
    back = [(j, i) for i, j in ahead]
    start = state
    current = state
    first, other = call(pack_kernel, [], [state], (FIRST, OTHER), "pack")
    for section in range(2):
        second = section == 1
        first_in = lax.ppermute(first, AXES, ahead)
        other_in = lax.ppermute(other, AXES, back)
        partial = call(
            functools.partial(volume_kernel, second=second),
            [mean_flow],
            [start, current] if second else [current],
            (BLOCK,),
            "volume",
            flops=10**8,
        )
        message = call(
            functools.partial(mortar_kernel, section=section),
            [frac_index],
            [first, first_in],
            (TRACE,),
            "mortar",
        )
        plus = rotated(message, sector_offset[section], count)
        results = call(
            functools.partial(close_kernel, second=second),
            [mean_flow],
            [partial, current, first_in, other_in, plus],
            (BLOCK,) if second else (BLOCK, FIRST, OTHER),
            "close",
            keep=not second,
        )
        if not second:
            current, first, other = results
    return results


def solution(mesh):
    in_specs = (P(None, None, None, None, ("blk", "sector")), P(), P(), P())
    out_specs = P(None, None, None, None, ("blk", "sector"))
    return jax.shard_map(
        per_device, mesh=mesh, in_specs=in_specs, out_specs=out_specs, check_vma=False
    )
```

```python
import functools
import math

import jax
import jax.numpy as jnp
import numpy as np
from jax import lax
from jax.experimental import pallas as pl
from jax.experimental.pallas import tpu as pltpu
from jax.sharding import PartitionSpec as P

FRACS = 4
EA = 8
ER = 4
EZ = 4
VARS = 5
NODES = 6
LANES = EA * ER * EZ
SLAB = EA * ER
AXES = ("blk", "sector")
TIME_STEP = 0.02
LIFT = NODES * (NODES - 1) / 2.0
HIGH = 16
LOW = 8
FACE_TILES = VARS
TRACE_TILES = 8


def lobatto_points():
    outer = math.sqrt(1.0 / 3.0 + 2.0 * math.sqrt(7.0) / 21.0)
    inner = math.sqrt(1.0 / 3.0 - 2.0 * math.sqrt(7.0) / 21.0)
    return np.array([-1.0, -outer, -inner, inner, outer, 1.0])


def derivative_matrix(points):
    number = points.shape[0]
    bary = [
        1.0 / np.prod([points[i] - points[j] for j in range(number) if j != i])
        for i in range(number)
    ]
    matrix = np.zeros((number, number))
    for i in range(number):
        for j in range(number):
            if i != j:
                matrix[i, j] = bary[j] / bary[i] / (points[i] - points[j])
        matrix[i, i] = -np.sum(matrix[i])
    return matrix


POINTS = lobatto_points()
DERIV = derivative_matrix(POINTS).astype(np.float32)


def iota(axis):
    return lax.broadcasted_iota(jnp.int32, (NODES, LANES), axis)


def by_row(values):
    row = iota(0)
    result = jnp.full((NODES, LANES), float(values[0]), jnp.float32)
    for at in range(1, NODES):
        result = jnp.where(row == at, float(values[at]), result)
    return result


def azimuth_scale():
    radial = lax.shift_right_logical(iota(1), 3) & (ER - 1)
    result = jnp.full((NODES, LANES), 2.0 / (1.0 + 0.5 / ER), jnp.float32)
    for at in range(1, ER):
        result = jnp.where(radial == at, 2.0 / (1.0 + (at + 0.5) / ER), result)
    return result


def spread(flow, direction):
    return jnp.maximum(
        jnp.abs(flow[0, direction - 1]), jnp.abs(flow[1, direction - 1])
    ) + jnp.maximum(flow[0, 3], flow[1, 3])


def turned(tile, by):
    by = by % LANES
    return pltpu.roll(tile, by, 1) if by else tile


def jump_rates(jumps, direction, normal, speed, sound, wide, factor):
    along = -factor * 0.5 * (normal * speed - wide)
    across = -factor * 0.5 * normal * sound
    rates = [along * jump for jump in jumps]
    rates[0] = rates[0] + across * jumps[direction]
    rates[direction] = rates[direction] + across * jumps[0]
    return rates


def coefficient(index, column):
    value = jnp.float32(DERIV[0, column])
    for at in range(1, NODES):
        value = jnp.where(index == at, jnp.float32(DERIV[at, column]), value)
    return value


def volume_kernel(flow, *refs, second):
    if second:
        start, x, out = refs
    else:
        x, out = refs
    gain = TIME_STEP * (0.5 if second else 1.0)
    row = lax.axis_index("blk")
    rotor = (row == 0).astype(jnp.float32)
    speed = [flow[row, at] for at in range(3)]
    sound = flow[row, 3]
    wide = [spread(flow, at + 1) for at in range(3)]
    lane = iota(1)
    slot = lane & (EA - 1)
    radial = lax.shift_right_logical(lane, 3) & (ER - 1)
    layer = lax.shift_right_logical(lane, 5)
    scale = azimuth_scale()
    columns = [scale * by_row(DERIV[:, at]) for at in range(NODES)]
    c_axial, c_radial, c_azimuth = -gain * 2.0 * speed[2], -gain * 2.0 * speed[1], -gain * speed[0]
    c_sound, c_sound2 = -gain * sound, -gain * 2.0 * sound
    lift = gain * LIFT * 2.0

    def at_layer(i, carry):
        axial = [coefficient(i, j) for j in range(NODES)]
        for b in range(NODES):
            rates = [None] * VARS
            grads = []
            for v in range(VARS):
                ga = axial[0] * x[v, 0, b]
                gb = DERIV[b, 0] * x[v, i, 0]
                gc = columns[0] * x[v, i, b, 0:1, :]
                for j in range(1, NODES):
                    ga = ga + axial[j] * x[v, j, b]
                    gb = gb + DERIV[b, j] * x[v, i, j]
                    gc = gc + columns[j] * x[v, i, b, j : j + 1, :]
                rates[v] = c_axial * ga + c_radial * gb + c_azimuth * gc
                if v == 0:
                    grads = [gc, gb, ga]
                elif v == 1:
                    rates[0] = rates[0] + c_sound * gc
                    rates[1] = rates[1] + c_sound * grads[0]
                elif v == 2:
                    rates[0] = rates[0] + c_sound2 * gb
                    rates[2] = rates[2] + c_sound2 * grads[1]
                elif v == 3:
                    rates[0] = rates[0] + c_sound2 * ga
                    rates[3] = rates[3] + c_sound2 * grads[2]
            if b == 0 or b == NODES - 1:
                normal, by, wall = (-1.0, EA, 0) if b == 0 else (1.0, -EA, ER - 1)
                jumps = []
                for v in range(VARS):
                    inside = x[v, i, b]
                    gap = turned(x[v, i, NODES - 1 - b], by) - inside
                    at_wall = -2.0 * inside if v == 2 else jnp.zeros_like(inside)
                    jumps.append(jnp.where(radial == wall, at_wall, gap))
                terms = jump_rates(jumps, 2, normal, speed[1], sound, wide[1], lift)
                rates = [rate + term for rate, term in zip(rates, terms)]
            for v in range(VARS):
                base = x[v, i, b]
                if second:
                    base = 0.5 * (start[v, i, b] + base)
                out[v, i, b] = base + rates[v]
        left = [x[v, i, :, 0, :] for v in range(VARS)]
        right = [x[v, i, :, NODES - 1, :] for v in range(VARS)]
        lower = [
            jnp.where(slot == 0, 0.0, turned(right[v], 1) - left[v]) for v in range(VARS)
        ]
        upper = [
            jnp.where(slot == EA - 1, 0.0, turned(left[v], -1) - right[v]) for v in range(VARS)
        ]
        factor = gain * LIFT * scale
        lower = jump_rates(lower, 1, -1.0, speed[0], sound, wide[0], factor)
        upper = jump_rates(upper, 1, 1.0, speed[0], sound, wide[0], factor)
        for v in range(VARS):
            out[v, i, :, 0, :] = out[v, i, :, 0, :] + lower[v]
            out[v, i, :, NODES - 1, :] = out[v, i, :, NODES - 1, :] + upper[v]
        return carry

    lax.fori_loop(0, NODES, at_layer, 0)

    def at_radial(b, carry):
        for i in (0, NODES - 1):
            normal, by, end = (-1.0, SLAB, 0) if i == 0 else (1.0, -SLAB, EZ - 1)
            keep = rotor if i == 0 else 1.0 - rotor
            jumps = []
            for v in range(VARS):
                inside = x[v, i, b]
                gap = turned(x[v, NODES - 1 - i, b], by) - inside
                jumps.append(jnp.where(layer == end, -keep * inside, gap))
            terms = jump_rates(jumps, 3, normal, speed[2], sound, wide[2], lift)
            for v in range(VARS):
                out[v, i, b] = out[v, i, b] + terms[v]
        return carry

    lax.fori_loop(0, NODES, at_radial, 0)


def pack(x, first, other):
    is_rotor = lax.axis_index("blk") == 0
    slot = iota(1) & (EA - 1)
    group = lax.shift_right_logical(iota(1), 5)
    zeros = jnp.zeros((NODES, LANES), jnp.float32)
    for v in range(VARS):
        low, high = zeros, zeros
        for a in range(NODES):
            low = jnp.where(slot == a, turned(x[v, a, :, 0, :], a), low)
            high = jnp.where(slot == a, turned(x[v, a, :, NODES - 1, :], a - EA + 1), high)
        first[v, 0:NODES, :] = jnp.where(is_rotor, high, low)
        other[v, 0:NODES, :] = jnp.where(is_rotor, low, high)

    def trace(plane, start):
        for p in range(TRACE_TILES):
            tile = zeros
            for o in range(EZ):
                t = p * EZ + o
                if t < VARS * NODES:
                    v, b = t // NODES, t % NODES
                    tile = jnp.where(group == o, turned(x[v, plane, b], SLAB * o - start), tile)
            first[FACE_TILES + p, 0:NODES, :] = tile

    @pl.when(is_rotor)
    def _():
        trace(NODES - 1, LANES - SLAB)

    @pl.when(jnp.logical_not(is_rotor))
    def _():
        trace(0, 0)


def pack_kernel(state, flow_in, offset_in, frac_in, *refs):
    x, first, other, flow, frac = refs[:5]
    turns, (offset, *arrivals) = refs[5:9], refs[9:]
    pairs = ((state, x), (flow_in, flow), (offset_in, offset), (frac_in, frac))
    copies = [pltpu.make_async_copy(*pair, sem) for pair, sem in zip(pairs, arrivals)]
    for copy in copies:
        copy.start()
    for copy in copies[1:]:
        copy.wait()
    for section in range(2):
        turns[2 * section][0] = lax.shift_right_logical(offset[section], 3)
        turns[2 * section + 1][0] = offset[section] & (LOW - 1)
    copies[0].wait()
    pack(x, first, other)


def stay_kernel(source, target, done):
    copy = pltpu.make_async_copy(source, target, done)
    copy.start()
    copy.wait()


def mortar_kernel(frac, own, beyond, out, *, section):
    is_rotor = lax.axis_index("blk") == 0
    index = frac[section]
    whole = lax.shift_right_logical(index, 2)
    part = (index & (FRACS - 1)).astype(jnp.float32) * (1.0 / FRACS)
    begin = jnp.where(is_rotor, EA - 1 - whole, whole)
    scaled = by_row((POINTS + 1.0) / 2.0)
    for_stator = scaled - part
    for_rotor = scaled + part
    at = jnp.where(is_rotor, for_stator, for_rotor)
    upper = jnp.where(
        is_rotor, (scaled > part).astype(jnp.int32), (for_rotor >= 1.0).astype(jnp.int32)
    )
    step = jnp.where(is_rotor, 1 - upper, -upper).astype(jnp.float32)
    is_upper = upper == 1
    local = (at + step) * 2.0 - 1.0
    weights = []
    for s in range(NODES):
        weight = jnp.ones((NODES, LANES), jnp.float32)
        for j in range(NODES):
            if j != s:
                weight = weight * ((local - float(POINTS[j])) * float(1.0 / (POINTS[s] - POINTS[j])))
        weights.append(weight)
    slot = iota(1) & (EA - 1)

    def window(lead, trail, begin):
        return jnp.where(
            slot + begin < EA,
            pltpu.roll(lead, (LANES - begin) & (LANES - 1), 1),
            pltpu.roll(trail, (LANES + EA - begin) & (LANES - 1), 1),
        )

    for p in range(TRACE_TILES):
        mine = own[FACE_TILES + p, 0:NODES, :]
        theirs = beyond[FACE_TILES + p, 0:NODES, :]
        lead = jnp.where(is_rotor, theirs, mine)
        trail = jnp.where(is_rotor, mine, theirs)
        low = window(lead, trail, begin)
        high = window(lead, trail, begin + 1)
        total = None
        for s in range(NODES):
            pick = jnp.where(
                is_upper,
                jnp.broadcast_to(high[s : s + 1, :], (NODES, LANES)),
                jnp.broadcast_to(low[s : s + 1, :], (NODES, LANES)),
            )
            total = weights[s] * pick if total is None else total + weights[s] * pick
        out[p, 0:NODES, :] = total


def close_kernel(flow, acc, x, first, other, first_own, other_own, plus, *refs, second):
    if second:
        target, out, arrived, inner, bottom_sent, top_sent, arrival = refs
        messages = ()
    else:
        out, *messages, arrived, arrival = refs
    fetch = pltpu.make_async_copy(plus, arrived, arrival)
    fetch.start()
    gain = TIME_STEP * (0.5 if second else 1.0)
    row = lax.axis_index("blk")
    is_rotor = row == 0
    speed = [flow[row, at] for at in range(3)]
    sound = flow[row, 3]
    far_speed, far_sound = flow[1 - row, 2], flow[1 - row, 3]
    wide = [spread(flow, at + 1) for at in range(3)]
    lane = iota(1)
    slot = lane & (EA - 1)
    layer = lax.shift_right_logical(lane, 5)
    factor = gain * LIFT * azimuth_scale()
    lower, upper = [], []
    for v in range(VARS):
        one = first[v, 0:NODES, :] - other_own[v, 0:NODES, :]
        two = other[v, 0:NODES, :] - first_own[v, 0:NODES, :]
        lower.append(jnp.where(is_rotor, one, two))
        upper.append(jnp.where(is_rotor, two, one))
    lower = jump_rates(lower, 1, -1.0, speed[0], sound, wide[0], factor)
    upper = jump_rates(upper, 1, 1.0, speed[0], sound, wide[0], factor)

    def at_layer(i, carry):
        for v in range(VARS):
            out[v, i] = acc[v, i]
            west = pltpu.roll(lower[v], (LANES - i) & (LANES - 1), 1)
            east = pltpu.roll(upper[v], EA - 1 - i, 1)
            out[v, i, :, 0, :] = acc[v, i, :, 0, :] + jnp.where(slot == 0, west, 0.0)
            last = acc[v, i, :, NODES - 1, :] + jnp.where(slot == EA - 1, east, 0.0)
            out[v, i, :, NODES - 1, :] = last
        return carry

    lax.fori_loop(1, NODES - 1, at_layer, 0)
    if second:
        inside = (slice(None), slice(1, NODES - 1))
        send = pltpu.make_async_copy(out.at[inside], target.at[inside], inner)
        send.start()
    lax.fori_loop(0, 2, lambda side, carry: at_layer(side * (NODES - 1), carry), 0)
    fetch.wait()

    def interface(plane, start, normal):
        scale = -gain * LIFT * 2.0
        mine = scale * 0.5 * (wide[2] - normal * speed[2])
        theirs = scale * 0.5 * (normal * far_speed - wide[2])
        cross_mine = -scale * 0.5 * normal * sound
        cross_theirs = scale * 0.5 * normal * far_sound
        for b in range(NODES):
            inside = [x[v, plane, b] for v in range(VARS)]
            outside = []
            for v in range(VARS):
                p, o = divmod(v * NODES + b, EZ)
                outside.append(turned(arrived[p, 0:NODES, :], start - SLAB * o))
            for v in range(VARS):
                term = mine * inside[v] + theirs * outside[v]
                if v == 0 or v == 3:
                    term = term + (cross_mine * inside[3 - v] + cross_theirs * outside[3 - v])
                out[v, plane, b] = out[v, plane, b] + jnp.where(layer == start // SLAB, term, 0.0)

    @pl.when(is_rotor)
    def _():
        interface(NODES - 1, LANES - SLAB, 1.0)

    @pl.when(jnp.logical_not(is_rotor))
    def _():
        interface(0, 0, -1.0)

    if messages:
        pack(out, *messages)
    if second:
        bottom = pltpu.make_async_copy(out.at[:, 0], target.at[:, 0], bottom_sent)
        top = pltpu.make_async_copy(out.at[:, NODES - 1], target.at[:, NODES - 1], top_sent)
        bottom.start()
        top.start()
        send.wait()
        bottom.wait()
        top.wait()


VMEM = pl.BlockSpec(memory_space=pltpu.VMEM)
SMEM = pl.BlockSpec(memory_space=pltpu.SMEM)
HBM = pl.BlockSpec(memory_space=pltpu.HBM)
BLOCK = (VARS, NODES, NODES, NODES, LANES)
FIRST = (FACE_TILES + TRACE_TILES, 8, LANES)
OTHER = (FACE_TILES, 8, LANES)
TRACE = (TRACE_TILES, 8, LANES)


def call(body, scalars, arrays, shapes, name, flops=1000, **more):
    arrays = [pltpu.with_memory_space_constraint(array, pltpu.VMEM) for array in arrays]
    outs = [pltpu.VMEM(shape, jnp.float32) for shape in shapes] + more.pop("more_outs", [])
    specs = [VMEM for _ in shapes] + more.pop("more_specs", [])
    others = [
        pltpu.with_memory_space_constraint(array, pltpu.HBM) for array in more.pop("others", [])
    ]
    results = pl.pallas_call(
        body,
        in_specs=[SMEM] * len(scalars) + [VMEM] * len(arrays) + [HBM] * len(others),
        out_specs=tuple(specs),
        out_shape=tuple(outs),
        cost_estimate=pl.CostEstimate(flops=flops, transcendentals=0, bytes_accessed=10**6),
        compiler_params=pltpu.CompilerParams(vmem_limit_bytes=16 * 2**20),
        name=name,
        **more,
    )(*scalars, *arrays, *others)
    return results if len(results) > 1 else results[0]


def stay(array):
    return pl.pallas_call(
        stay_kernel,
        in_specs=[HBM],
        out_specs=HBM,
        out_shape=jax.ShapeDtypeStruct(TRACE, jnp.float32),
        scratch_shapes=[pltpu.SemaphoreType.DMA(())],
        name="stay",
    )(array)


def rotated(message, high, low, count):
    def far(turn):
        shift = LOW * turn
        pairs = [(i, count + (i + shift) % count) for i in range(count)]
        pairs += [(count + (i + shift) % count, i) for i in range(count)]
        return lambda array: lax.ppermute(array, AXES, pairs)

    def near(turn):
        if turn == 0:
            return stay
        pairs = [(i, (i - turn) % count) for i in range(count)]
        pairs += [(count + i, count + (i + turn) % count) for i in range(count)]
        return lambda array: lax.ppermute(array, AXES, pairs)

    message = lax.switch(high, [far(at) for at in range(count // LOW)], message)
    return lax.switch(low, [near(at) for at in range(LOW)], message)


def per_device(state, mean_flow, sector_offset, frac_index):
    count = lax.axis_size("sector")
    ahead = [(i, (i + 1) % count) for i in range(count)]
    ahead += [(count + (i + 1) % count, count + i) for i in range(count)]
    back = [(j, i) for i, j in ahead]
    start, first, other, flow, frac, *turns = call(
        pack_kernel,
        [],
        [],
        (BLOCK, FIRST, OTHER),
        "pack",
        others=[state, mean_flow, sector_offset, frac_index],
        more_outs=[pltpu.SMEM((2, 4), jnp.float32), pltpu.SMEM((2,), jnp.int32)]
        + [pltpu.SMEM((1,), jnp.int32)] * 4,
        more_specs=[SMEM] * 6,
        scratch_shapes=[pltpu.SMEM((2,), jnp.int32)] + [pltpu.SemaphoreType.DMA(())] * 4,
    )
    current = start
    flow = pltpu.with_memory_space_constraint(flow, pltpu.SMEM)
    frac = pltpu.with_memory_space_constraint(frac, pltpu.SMEM)
    for section in range(2):
        second = section == 1
        first_in = lax.ppermute(first, AXES, ahead)
        other_in = lax.ppermute(other, AXES, back)
        partial = call(
            functools.partial(volume_kernel, second=second),
            [flow],
            [start, current] if second else [current],
            (BLOCK,),
            "volume",
            flops=10**8,
        )
        message = call(
            functools.partial(mortar_kernel, section=section),
            [frac],
            [first, first_in],
            (TRACE,),
            "mortar",
        )
        high, low = turns[2 * section].reshape(()), turns[2 * section + 1].reshape(())
        plus = rotated(message, high, low, count)
        scratch = [pltpu.VMEM(TRACE, jnp.float32)]
        if second:
            scratch = [pltpu.VMEM(BLOCK, jnp.float32)] + scratch
            semaphores = [pltpu.SemaphoreType.DMA(())] * 4
            more = {
                "more_outs": [jax.ShapeDtypeStruct(BLOCK, jnp.float32)],
                "more_specs": [HBM],
            }
        else:
            semaphores = [pltpu.SemaphoreType.DMA(())]
            more = {}
        results = call(
            functools.partial(close_kernel, second=second),
            [flow],
            [partial, current, first_in, other_in, first, other],
            () if second else (BLOCK, FIRST, OTHER),
            "close",
            others=[plus],
            scratch_shapes=scratch + semaphores,
            **more,
        )
        if not second:
            current, first, other = results
    return results


def solution(mesh):
    in_specs = (P(None, None, None, None, ("blk", "sector")), P(), P(), P())
    out_specs = P(None, None, None, None, ("blk", "sector"))
    return jax.shard_map(
        per_device, mesh=mesh, in_specs=in_specs, out_specs=out_specs, check_vma=False
    )
```

```python
import functools
import math

import jax
import jax.numpy as jnp
import numpy as np
from jax import lax
from jax.experimental import pallas as pl
from jax.experimental.pallas import tpu as pltpu
from jax.sharding import PartitionSpec as P

FRACS = 4
EA = 8
ER = 4
EZ = 4
VARS = 5
NODES = 6
LANES = EA * ER * EZ
SLAB = EA * ER
AXES = ("blk", "sector")
TIME_STEP = 0.02
LIFT = NODES * (NODES - 1) / 2.0
HIGH = 16
LOW = 8
FACE_TILES = VARS
TRACE_TILES = 8


def lobatto_points():
    outer = math.sqrt(1.0 / 3.0 + 2.0 * math.sqrt(7.0) / 21.0)
    inner = math.sqrt(1.0 / 3.0 - 2.0 * math.sqrt(7.0) / 21.0)
    return np.array([-1.0, -outer, -inner, inner, outer, 1.0])


def derivative_matrix(points):
    number = points.shape[0]
    bary = [
        1.0 / np.prod([points[i] - points[j] for j in range(number) if j != i])
        for i in range(number)
    ]
    matrix = np.zeros((number, number))
    for i in range(number):
        for j in range(number):
            if i != j:
                matrix[i, j] = bary[j] / bary[i] / (points[i] - points[j])
        matrix[i, i] = -np.sum(matrix[i])
    return matrix


POINTS = lobatto_points()
DERIV = derivative_matrix(POINTS).astype(np.float32)
HALF = NODES // 2
EVEN = ((DERIV[:HALF, :HALF] + DERIV[:HALF, : HALF - 1 : -1]) / 2).astype(np.float32)
ODD = ((DERIV[:HALF, :HALF] - DERIV[:HALF, : HALF - 1 : -1]) / 2).astype(np.float32)


def iota(axis):
    return lax.broadcasted_iota(jnp.int32, (NODES, LANES), axis)


def by_row(values):
    row = iota(0)
    result = jnp.full((NODES, LANES), float(values[0]), jnp.float32)
    for at in range(1, NODES):
        result = jnp.where(row == at, float(values[at]), result)
    return result


def azimuth_scale():
    radial = lax.shift_right_logical(iota(1), 3) & (ER - 1)
    result = jnp.full((NODES, LANES), 2.0 / (1.0 + 0.5 / ER), jnp.float32)
    for at in range(1, ER):
        result = jnp.where(radial == at, 2.0 / (1.0 + (at + 0.5) / ER), result)
    return result


def spread(flow, direction):
    return jnp.maximum(
        jnp.abs(flow[0, direction - 1]), jnp.abs(flow[1, direction - 1])
    ) + jnp.maximum(flow[0, 3], flow[1, 3])


def turned(array, by):
    by = by % LANES
    return pltpu.roll(array, by, 1) if by else array


def tile(at):
    return slice(at * NODES, (at + 1) * NODES), slice(None)


def jump_rates(jumps, direction, normal, speed, sound, wide, factor):
    along = -factor * 0.5 * (normal * speed - wide)
    across = -factor * 0.5 * normal * sound
    rates = [along * jump for jump in jumps]
    rates[0] = rates[0] + across * jumps[direction]
    rates[direction] = rates[direction] + across * jumps[0]
    return rates


def coefficient(index, column):
    value = jnp.float32(DERIV[0, column])
    for at in range(1, NODES):
        value = jnp.where(index == at, jnp.float32(DERIV[at, column]), value)
    return value


def volume_kernel(flow, *refs, second):
    if second:
        start, x, out = refs
    else:
        x, out = refs
    gain = TIME_STEP * (0.5 if second else 1.0)
    row = lax.axis_index("blk")
    rotor = (row == 0).astype(jnp.float32)
    speed = [flow[row, at] for at in range(3)]
    sound = flow[row, 3]
    wide = [spread(flow, at + 1) for at in range(3)]
    lane = iota(1)
    slot = lane & (EA - 1)
    radial = lax.shift_right_logical(lane, 3) & (ER - 1)
    layer = lax.shift_right_logical(lane, 5)
    scale = azimuth_scale()
    columns = [scale * by_row(DERIV[:, at]) for at in range(NODES)]
    c_axial, c_radial, c_azimuth = -gain * 2.0 * speed[2], -gain * 2.0 * speed[1], -gain * speed[0]
    c_sound, c_sound2 = -gain * sound, -gain * 2.0 * sound
    lift = gain * LIFT * 2.0

    row_of = iota(0)
    bottom = (row_of == 0) & (slot != 0)
    top = (row_of == NODES - 1) & (slot != EA - 1)
    lifted = -0.5 * gain * LIFT * scale
    side_along = jnp.where(
        bottom, lifted * (-speed[0] - wide[0]), jnp.where(top, lifted * (speed[0] - wide[0]), 0.0)
    )
    side_across = jnp.where(bottom, lifted * -sound, jnp.where(top, lifted * sound, 0.0))

    def at_layer(i, carry):
        axial = [coefficient(i, j) for j in range(NODES)]
        even = [[x[v, i, j] + x[v, i, NODES - 1 - j] for j in range(HALF)] for v in range(VARS)]
        odd = [[x[v, i, j] - x[v, i, NODES - 1 - j] for j in range(HALF)] for v in range(VARS)]
        for m in range(HALF):
            radials = []
            for v in range(VARS):
                sums = EVEN[m, 0] * even[v][0]
                gaps = ODD[m, 0] * odd[v][0]
                for j in range(1, HALF):
                    sums = sums + EVEN[m, j] * even[v][j]
                    gaps = gaps + ODD[m, j] * odd[v][j]
                radials.append((gaps + sums, gaps - sums))
            for side, b in enumerate((m, NODES - 1 - m)):
                at_tile(i, b, axial, [radial_pair[side] for radial_pair in radials])
        return carry

    def at_tile(i, b, axial, gradients):
        rates = [None] * VARS
        grads = []
        sides = []
        for v in range(VARS):
            here = x[v, i, b]
            ga = axial[0] * x[v, 0, b]
            gb = gradients[v]
            gc = columns[0] * x[v, i, b, 0:1, :]
            for j in range(1, NODES):
                ga = ga + axial[j] * x[v, j, b]
                gc = gc + columns[j] * x[v, i, b, j : j + 1, :]
            from_west = jnp.broadcast_to(x[v, i, b, NODES - 1 : NODES, :], (NODES, LANES))
            from_east = jnp.broadcast_to(x[v, i, b, 0:1, :], (NODES, LANES))
            beside = jnp.where(row_of == 0, turned(from_west, 1), turned(from_east, -1))
            sides.append(beside - here)
            rates[v] = c_axial * ga + c_radial * gb + c_azimuth * gc + side_along * sides[v]
            if v == 0:
                grads = [gc, gb, ga]
            elif v == 1:
                rates[0] = rates[0] + c_sound * gc + side_across * sides[1]
                rates[1] = rates[1] + c_sound * grads[0] + side_across * sides[0]
            elif v == 2:
                rates[0] = rates[0] + c_sound2 * gb
                rates[2] = rates[2] + c_sound2 * grads[1]
            elif v == 3:
                rates[0] = rates[0] + c_sound2 * ga
                rates[3] = rates[3] + c_sound2 * grads[2]
        if b == 0 or b == NODES - 1:
            normal, by, wall = (-1.0, EA, 0) if b == 0 else (1.0, -EA, ER - 1)
            jumps = []
            for v in range(VARS):
                inside = x[v, i, b]
                gap = turned(x[v, i, NODES - 1 - b], by) - inside
                at_wall = -2.0 * inside if v == 2 else jnp.zeros_like(inside)
                jumps.append(jnp.where(radial == wall, at_wall, gap))
            terms = jump_rates(jumps, 2, normal, speed[1], sound, wide[1], lift)
            rates = [rate + term for rate, term in zip(rates, terms)]
        for v in range(VARS):
            base = x[v, i, b]
            if second:
                base = 0.5 * (start[v, i, b] + base)
            out[v, i, b] = base + rates[v]

    lax.fori_loop(0, NODES, at_layer, 0)

    def at_radial(b, carry):
        for i in (0, NODES - 1):
            normal, by, end = (-1.0, SLAB, 0) if i == 0 else (1.0, -SLAB, EZ - 1)
            keep = rotor if i == 0 else 1.0 - rotor
            jumps = []
            for v in range(VARS):
                inside = x[v, i, b]
                gap = turned(x[v, NODES - 1 - i, b], by) - inside
                jumps.append(jnp.where(layer == end, -keep * inside, gap))
            terms = jump_rates(jumps, 3, normal, speed[2], sound, wide[2], lift)
            for v in range(VARS):
                out[v, i, b] = out[v, i, b] + terms[v]
        return carry

    lax.fori_loop(0, NODES, at_radial, 0)


def pack(x, first, other):
    is_rotor = lax.axis_index("blk") == 0
    slot = iota(1) & (EA - 1)
    group = lax.shift_right_logical(iota(1), 5)
    zeros = jnp.zeros((NODES, LANES), jnp.float32)
    for v in range(VARS):
        low, high = zeros, zeros
        for a in range(NODES):
            low = jnp.where(slot == a, turned(x[v, a, :, 0, :], a), low)
            high = jnp.where(slot == a, turned(x[v, a, :, NODES - 1, :], a - EA + 1), high)
        first[tile(v)] = jnp.where(is_rotor, high, low)
        other[tile(v)] = jnp.where(is_rotor, low, high)

    def trace(plane, start):
        for p in range(TRACE_TILES):
            packed = zeros
            for o in range(EZ):
                t = p * EZ + o
                if t < VARS * NODES:
                    v, b = t // NODES, t % NODES
                    packed = jnp.where(group == o, turned(x[v, plane, b], SLAB * o - start), packed)
            first[tile(FACE_TILES + p)] = packed

    @pl.when(is_rotor)
    def _():
        trace(NODES - 1, LANES - SLAB)

    @pl.when(jnp.logical_not(is_rotor))
    def _():
        trace(0, 0)


def pack_kernel(state, flow_in, offset_in, frac_in, *refs):
    x, first, other, flow, frac = refs[:5]
    turns, (offset, *arrivals) = refs[5:9], refs[9:]
    pairs = [(flow_in, flow), (offset_in, offset), (frac_in, frac)]
    pairs.append((state, x))
    copies = [pltpu.make_async_copy(*pair, sem) for pair, sem in zip(pairs, arrivals)]
    for copy in copies:
        copy.start()
    for copy in copies[:3]:
        copy.wait()
    for section in range(2):
        turns[2 * section][0] = lax.shift_right_logical(offset[section], 3)
        turns[2 * section + 1][0] = offset[section] & (LOW - 1)
    copies[3].wait()
    pack(x, first, other)


def stay_kernel(source, target, done):
    copy = pltpu.make_async_copy(source, target, done)
    copy.start()
    copy.wait()


def mortar_kernel(frac, own, beyond, out, *, section):
    is_rotor = lax.axis_index("blk") == 0
    index = frac[section]
    whole = lax.shift_right_logical(index, 2)
    part = (index & (FRACS - 1)).astype(jnp.float32) * (1.0 / FRACS)
    begin = jnp.where(is_rotor, EA - 1 - whole, whole)
    scaled = by_row((POINTS + 1.0) / 2.0)
    for_stator = scaled - part
    for_rotor = scaled + part
    at = jnp.where(is_rotor, for_stator, for_rotor)
    upper = jnp.where(
        is_rotor, (scaled > part).astype(jnp.int32), (for_rotor >= 1.0).astype(jnp.int32)
    )
    step = jnp.where(is_rotor, 1 - upper, -upper).astype(jnp.float32)
    is_upper = upper == 1
    local = (at + step) * 2.0 - 1.0
    weights = []
    for s in range(NODES):
        weight = jnp.ones((NODES, LANES), jnp.float32)
        for j in range(NODES):
            if j != s:
                weight = weight * ((local - float(POINTS[j])) * float(1.0 / (POINTS[s] - POINTS[j])))
        weights.append(weight)
    slot = iota(1) & (EA - 1)

    def window(lead, trail, begin):
        return jnp.where(
            slot + begin < EA,
            pltpu.roll(lead, (LANES - begin) & (LANES - 1), 1),
            pltpu.roll(trail, (LANES + EA - begin) & (LANES - 1), 1),
        )

    for p in range(TRACE_TILES):
        mine = own[tile(FACE_TILES + p)]
        theirs = beyond[tile(FACE_TILES + p)]
        lead = jnp.where(is_rotor, theirs, mine)
        trail = jnp.where(is_rotor, mine, theirs)
        low = window(lead, trail, begin)
        high = window(lead, trail, begin + 1)
        total = None
        for s in range(NODES):
            pick = jnp.where(
                is_upper,
                jnp.broadcast_to(high[s : s + 1, :], (NODES, LANES)),
                jnp.broadcast_to(low[s : s + 1, :], (NODES, LANES)),
            )
            total = weights[s] * pick if total is None else total + weights[s] * pick
        out[tile(p)] = total


def close_kernel(flow, acc, x, first, other, first_own, other_own, plus, *refs, second):
    if second:
        target, out, arrived, inner, bottom_sent, top_sent, arrival = refs
        messages = ()
    else:
        out, *messages, arrived, arrival = refs
    fetch = pltpu.make_async_copy(plus, arrived, arrival)
    fetch.start()
    gain = TIME_STEP * (0.5 if second else 1.0)
    row = lax.axis_index("blk")
    is_rotor = row == 0
    speed = [flow[row, at] for at in range(3)]
    sound = flow[row, 3]
    far_speed, far_sound = flow[1 - row, 2], flow[1 - row, 3]
    wide = [spread(flow, at + 1) for at in range(3)]
    lane = iota(1)
    slot = lane & (EA - 1)
    layer = lax.shift_right_logical(lane, 5)
    factor = gain * LIFT * azimuth_scale()
    lower, upper = [], []
    for v in range(VARS):
        one = first[tile(v)] - other_own[tile(v)]
        two = other[tile(v)] - first_own[tile(v)]
        lower.append(jnp.where(is_rotor, one, two))
        upper.append(jnp.where(is_rotor, two, one))
    lower = jump_rates(lower, 1, -1.0, speed[0], sound, wide[0], factor)
    upper = jump_rates(upper, 1, 1.0, speed[0], sound, wide[0], factor)

    def at_layer(i, carry):
        for v in range(VARS):
            out[v, i] = acc[v, i]
            west = pltpu.roll(lower[v], (LANES - i) & (LANES - 1), 1)
            east = pltpu.roll(upper[v], EA - 1 - i, 1)
            out[v, i, :, 0, :] = acc[v, i, :, 0, :] + jnp.where(slot == 0, west, 0.0)
            last = acc[v, i, :, NODES - 1, :] + jnp.where(slot == EA - 1, east, 0.0)
            out[v, i, :, NODES - 1, :] = last
        return carry

    lax.fori_loop(1, NODES - 1, at_layer, 0)
    if second:
        inside = (slice(None), slice(1, NODES - 1))
        send = pltpu.make_async_copy(out.at[inside], target.at[inside], inner)
        send.start()
    lax.fori_loop(0, 2, lambda side, carry: at_layer(side * (NODES - 1), carry), 0)
    fetch.wait()

    def interface(plane, start, normal):
        scale = -gain * LIFT * 2.0
        mine = scale * 0.5 * (wide[2] - normal * speed[2])
        theirs = scale * 0.5 * (normal * far_speed - wide[2])
        cross_mine = -scale * 0.5 * normal * sound
        cross_theirs = scale * 0.5 * normal * far_sound
        for b in range(NODES):
            inside = [x[v, plane, b] for v in range(VARS)]
            outside = []
            for v in range(VARS):
                p, o = divmod(v * NODES + b, EZ)
                outside.append(turned(arrived[tile(p)], start - SLAB * o))
            for v in range(VARS):
                term = mine * inside[v] + theirs * outside[v]
                if v == 0 or v == 3:
                    term = term + (cross_mine * inside[3 - v] + cross_theirs * outside[3 - v])
                out[v, plane, b] = out[v, plane, b] + jnp.where(layer == start // SLAB, term, 0.0)

    @pl.when(is_rotor)
    def _():
        interface(NODES - 1, LANES - SLAB, 1.0)

    @pl.when(jnp.logical_not(is_rotor))
    def _():
        interface(0, 0, -1.0)

    if messages:
        pack(out, *messages)
    if second:
        bottom = pltpu.make_async_copy(out.at[:, 0], target.at[:, 0], bottom_sent)
        top = pltpu.make_async_copy(out.at[:, NODES - 1], target.at[:, NODES - 1], top_sent)
        bottom.start()
        top.start()
        send.wait()
        bottom.wait()
        top.wait()


VMEM = pl.BlockSpec(memory_space=pltpu.VMEM)
SMEM = pl.BlockSpec(memory_space=pltpu.SMEM)
HBM = pl.BlockSpec(memory_space=pltpu.HBM)
BLOCK = (VARS, NODES, NODES, NODES, LANES)
FIRST = (80, LANES)
OTHER = (32, LANES)
TRACE = (TRACE_TILES * NODES, LANES)


def call(body, scalars, arrays, shapes, name, flops=1000, **more):
    arrays = [pltpu.with_memory_space_constraint(array, pltpu.VMEM) for array in arrays]
    outs = [pltpu.VMEM(shape, jnp.float32) for shape in shapes] + more.pop("more_outs", [])
    specs = [VMEM for _ in shapes] + more.pop("more_specs", [])
    others = [
        pltpu.with_memory_space_constraint(array, pltpu.HBM) for array in more.pop("others", [])
    ]
    results = pl.pallas_call(
        body,
        in_specs=[SMEM] * len(scalars) + [VMEM] * len(arrays) + [HBM] * len(others),
        out_specs=tuple(specs),
        out_shape=tuple(outs),
        cost_estimate=pl.CostEstimate(flops=flops, transcendentals=0, bytes_accessed=10**6),
        compiler_params=pltpu.CompilerParams(vmem_limit_bytes=16 * 2**20),
        name=name,
        **more,
    )(*scalars, *arrays, *others)
    return results if len(results) > 1 else results[0]


def stay(array):
    return pl.pallas_call(
        stay_kernel,
        in_specs=[HBM],
        out_specs=HBM,
        out_shape=jax.ShapeDtypeStruct(TRACE, jnp.float32),
        scratch_shapes=[pltpu.SemaphoreType.DMA(())],
        name="stay",
    )(array)


def rotated(message, high, low, count):
    def far(turn):
        shift = LOW * turn
        pairs = [(i, count + (i + shift) % count) for i in range(count)]
        pairs += [(count + (i + shift) % count, i) for i in range(count)]
        return lambda array: lax.ppermute(array, AXES, pairs)

    def near(turn):
        if turn == 0:
            return stay
        pairs = [(i, (i - turn) % count) for i in range(count)]
        pairs += [(count + i, count + (i + turn) % count) for i in range(count)]
        return lambda array: lax.ppermute(array, AXES, pairs)

    message = lax.switch(high, [far(at) for at in range(count // LOW)], message)
    return lax.switch(low, [near(at) for at in range(LOW)], message)


def per_device(state, mean_flow, sector_offset, frac_index):
    count = lax.axis_size("sector")
    ahead = [(i, (i + 1) % count) for i in range(count)]
    ahead += [(count + (i + 1) % count, count + i) for i in range(count)]
    back = [(j, i) for i, j in ahead]
    start, first, other, flow, frac, *turns = call(
        pack_kernel,
        [],
        [],
        (BLOCK, FIRST, OTHER),
        "pack",
        others=[state, mean_flow, sector_offset, frac_index],
        more_outs=[pltpu.SMEM((2, 4), jnp.float32), pltpu.SMEM((2,), jnp.int32)]
        + [pltpu.SMEM((1,), jnp.int32)] * 4,
        more_specs=[SMEM] * 6,
        scratch_shapes=[pltpu.SMEM((2,), jnp.int32)] + [pltpu.SemaphoreType.DMA(())] * 4,
    )
    current = start
    flow = pltpu.with_memory_space_constraint(flow, pltpu.SMEM)
    frac = pltpu.with_memory_space_constraint(frac, pltpu.SMEM)
    for section in range(2):
        second = section == 1
        first_in = lax.ppermute(first, AXES, ahead)
        other_in = lax.ppermute(other, AXES, back)
        partial = call(
            functools.partial(volume_kernel, second=second),
            [flow],
            [start, current] if second else [current],
            (BLOCK,),
            "volume",
            flops=10**8,
        )
        message = call(
            functools.partial(mortar_kernel, section=section),
            [frac],
            [first, first_in],
            (TRACE,),
            "mortar",
        )
        high, low = turns[2 * section].reshape(()), turns[2 * section + 1].reshape(())
        plus = rotated(message, high, low, count)
        scratch = [pltpu.VMEM(TRACE, jnp.float32)]
        if second:
            scratch = [pltpu.VMEM(BLOCK, jnp.float32)] + scratch
            semaphores = [pltpu.SemaphoreType.DMA(())] * 4
            more = {
                "more_outs": [jax.ShapeDtypeStruct(BLOCK, jnp.float32)],
                "more_specs": [HBM],
            }
        else:
            semaphores = [pltpu.SemaphoreType.DMA(())]
            more = {}
        results = call(
            functools.partial(close_kernel, second=second),
            [flow],
            [partial, current, first_in, other_in, first, other],
            () if second else (BLOCK, FIRST, OTHER),
            "close",
            others=[plus],
            scratch_shapes=scratch + semaphores,
            **more,
        )
        if not second:
            current, first, other = results
    return results


def solution(mesh):
    in_specs = (P(None, None, None, None, ("blk", "sector")), P(), P(), P())
    out_specs = P(None, None, None, None, ("blk", "sector"))
    return jax.shard_map(
        per_device, mesh=mesh, in_specs=in_specs, out_specs=out_specs, check_vma=False
    )
```

```python
import functools
import math

import jax
import jax.numpy as jnp
import numpy as np
from jax import lax
from jax.experimental import pallas as pl
from jax.experimental.pallas import tpu as pltpu
from jax.sharding import PartitionSpec as P

FRACS = 4
EA = 8
ER = 4
EZ = 4
VARS = 5
NODES = 6
LANES = EA * ER * EZ
SLAB = EA * ER
AXES = ("blk", "sector")
TIME_STEP = 0.02
LIFT = NODES * (NODES - 1) / 2.0
HIGH = 16
LOW = 8
FACE_TILES = VARS
TRACE_TILES = 8


def lobatto_points():
    outer = math.sqrt(1.0 / 3.0 + 2.0 * math.sqrt(7.0) / 21.0)
    inner = math.sqrt(1.0 / 3.0 - 2.0 * math.sqrt(7.0) / 21.0)
    return np.array([-1.0, -outer, -inner, inner, outer, 1.0])


def derivative_matrix(points):
    number = points.shape[0]
    bary = [
        1.0 / np.prod([points[i] - points[j] for j in range(number) if j != i])
        for i in range(number)
    ]
    matrix = np.zeros((number, number))
    for i in range(number):
        for j in range(number):
            if i != j:
                matrix[i, j] = bary[j] / bary[i] / (points[i] - points[j])
        matrix[i, i] = -np.sum(matrix[i])
    return matrix


POINTS = lobatto_points()
DERIV = derivative_matrix(POINTS).astype(np.float32)
HALF = NODES // 2
EVEN = ((DERIV[:HALF, :HALF] + DERIV[:HALF, : HALF - 1 : -1]) / 2).astype(np.float32)
ODD = ((DERIV[:HALF, :HALF] - DERIV[:HALF, : HALF - 1 : -1]) / 2).astype(np.float32)


def iota(axis):
    return lax.broadcasted_iota(jnp.int32, (NODES, LANES), axis)


def by_row(values):
    row = iota(0)
    result = jnp.full((NODES, LANES), float(values[0]), jnp.float32)
    for at in range(1, NODES):
        result = jnp.where(row == at, float(values[at]), result)
    return result


def azimuth_scale():
    radial = lax.shift_right_logical(iota(1), 3) & (ER - 1)
    result = jnp.full((NODES, LANES), 2.0 / (1.0 + 0.5 / ER), jnp.float32)
    for at in range(1, ER):
        result = jnp.where(radial == at, 2.0 / (1.0 + (at + 0.5) / ER), result)
    return result


def spread(flow, direction):
    return jnp.maximum(
        jnp.abs(flow[0, direction - 1]), jnp.abs(flow[1, direction - 1])
    ) + jnp.maximum(flow[0, 3], flow[1, 3])


def turned(array, by):
    by = by % LANES
    return pltpu.roll(array, by, 1) if by else array


def tile(at):
    return slice(at * NODES, (at + 1) * NODES), slice(None)


def jump_rates(jumps, direction, normal, speed, sound, wide, factor):
    along = -factor * 0.5 * (normal * speed - wide)
    across = -factor * 0.5 * normal * sound
    rates = [along * jump for jump in jumps]
    rates[0] = rates[0] + across * jumps[direction]
    rates[direction] = rates[direction] + across * jumps[0]
    return rates


def coefficient(index, column):
    value = jnp.float32(DERIV[0, column])
    for at in range(1, NODES):
        value = jnp.where(index == at, jnp.float32(DERIV[at, column]), value)
    return value


def volume_kernel(flow, *refs, second):
    if second:
        start, x, out = refs
    else:
        x, out = refs
    gain = TIME_STEP * (0.5 if second else 1.0)
    row = lax.axis_index("blk")
    rotor = (row == 0).astype(jnp.float32)
    speed = [flow[row, at] for at in range(3)]
    sound = flow[row, 3]
    wide = [spread(flow, at + 1) for at in range(3)]
    lane = iota(1)
    slot = lane & (EA - 1)
    radial = lax.shift_right_logical(lane, 3) & (ER - 1)
    layer = lax.shift_right_logical(lane, 5)
    scale = azimuth_scale()
    columns = [scale * by_row(DERIV[:, at]) for at in range(NODES)]
    c_axial, c_radial, c_azimuth = -gain * 2.0 * speed[2], -gain * 2.0 * speed[1], -gain * speed[0]
    c_sound, c_sound2 = -gain * sound, -gain * 2.0 * sound
    lift = gain * LIFT * 2.0

    row_of = iota(0)
    bottom = (row_of == 0) & (slot != 0)
    top = (row_of == NODES - 1) & (slot != EA - 1)
    lifted = -0.5 * gain * LIFT * scale
    side_along = jnp.where(
        bottom, lifted * (-speed[0] - wide[0]), jnp.where(top, lifted * (speed[0] - wide[0]), 0.0)
    )
    side_across = jnp.where(bottom, lifted * -sound, jnp.where(top, lifted * sound, 0.0))

    def at_layer(i, carry):
        axial = [coefficient(i, j) for j in range(NODES)]
        even = [[x[v, i, j] + x[v, i, NODES - 1 - j] for j in range(HALF)] for v in range(VARS)]
        odd = [[x[v, i, j] - x[v, i, NODES - 1 - j] for j in range(HALF)] for v in range(VARS)]
        for m in range(HALF):
            radials = []
            for v in range(VARS):
                sums = EVEN[m, 0] * even[v][0]
                gaps = ODD[m, 0] * odd[v][0]
                for j in range(1, HALF):
                    sums = sums + EVEN[m, j] * even[v][j]
                    gaps = gaps + ODD[m, j] * odd[v][j]
                radials.append((gaps + sums, gaps - sums))
            for side, b in enumerate((m, NODES - 1 - m)):
                at_tile(i, b, axial, [radial_pair[side] for radial_pair in radials])
        return carry

    def at_tile(i, b, axial, gradients):
        rates = [None] * VARS
        grads = []
        sides = []
        for v in range(VARS):
            here = x[v, i, b]
            ga = axial[0] * x[v, 0, b]
            gb = gradients[v]
            gc = columns[0] * x[v, i, b, 0:1, :]
            for j in range(1, NODES):
                ga = ga + axial[j] * x[v, j, b]
                gc = gc + columns[j] * x[v, i, b, j : j + 1, :]
            from_west = jnp.broadcast_to(x[v, i, b, NODES - 1 : NODES, :], (NODES, LANES))
            from_east = jnp.broadcast_to(x[v, i, b, 0:1, :], (NODES, LANES))
            beside = jnp.where(row_of == 0, turned(from_west, 1), turned(from_east, -1))
            sides.append(beside - here)
            rates[v] = c_axial * ga + c_radial * gb + c_azimuth * gc + side_along * sides[v]
            if v == 0:
                grads = [gc, gb, ga]
            elif v == 1:
                rates[0] = rates[0] + c_sound * gc + side_across * sides[1]
                rates[1] = rates[1] + c_sound * grads[0] + side_across * sides[0]
            elif v == 2:
                rates[0] = rates[0] + c_sound2 * gb
                rates[2] = rates[2] + c_sound2 * grads[1]
            elif v == 3:
                rates[0] = rates[0] + c_sound2 * ga
                rates[3] = rates[3] + c_sound2 * grads[2]
        if b == 0 or b == NODES - 1:
            normal, by, wall = (-1.0, EA, 0) if b == 0 else (1.0, -EA, ER - 1)
            jumps = []
            for v in range(VARS):
                inside = x[v, i, b]
                gap = turned(x[v, i, NODES - 1 - b], by) - inside
                at_wall = -2.0 * inside if v == 2 else jnp.zeros_like(inside)
                jumps.append(jnp.where(radial == wall, at_wall, gap))
            terms = jump_rates(jumps, 2, normal, speed[1], sound, wide[1], lift)
            rates = [rate + term for rate, term in zip(rates, terms)]
        for v in range(VARS):
            base = x[v, i, b]
            if second:
                base = 0.5 * (start[v, i, b] + base)
            out[v, i, b] = base + rates[v]

    lax.fori_loop(0, NODES, at_layer, 0)

    def at_radial(b, carry):
        for i in (0, NODES - 1):
            normal, by, end = (-1.0, SLAB, 0) if i == 0 else (1.0, -SLAB, EZ - 1)
            keep = rotor if i == 0 else 1.0 - rotor
            jumps = []
            for v in range(VARS):
                inside = x[v, i, b]
                gap = turned(x[v, NODES - 1 - i, b], by) - inside
                jumps.append(jnp.where(layer == end, -keep * inside, gap))
            terms = jump_rates(jumps, 3, normal, speed[2], sound, wide[2], lift)
            for v in range(VARS):
                out[v, i, b] = out[v, i, b] + terms[v]
        return carry

    lax.fori_loop(0, NODES, at_radial, 0, unroll=True)


def pack(x, first, other):
    is_rotor = lax.axis_index("blk") == 0
    slot = iota(1) & (EA - 1)
    group = lax.shift_right_logical(iota(1), 5)
    zeros = jnp.zeros((NODES, LANES), jnp.float32)
    for v in range(VARS):
        low, high = zeros, zeros
        for a in range(NODES):
            low = jnp.where(slot == a, turned(x[v, a, :, 0, :], a), low)
            high = jnp.where(slot == a, turned(x[v, a, :, NODES - 1, :], a - EA + 1), high)
        first[tile(v)] = jnp.where(is_rotor, high, low)
        other[tile(v)] = jnp.where(is_rotor, low, high)

    def trace(plane, start):
        for p in range(TRACE_TILES):
            packed = zeros
            for o in range(EZ):
                t = p * EZ + o
                if t < VARS * NODES:
                    v, b = t // NODES, t % NODES
                    packed = jnp.where(group == o, turned(x[v, plane, b], SLAB * o - start), packed)
            first[tile(FACE_TILES + p)] = packed

    @pl.when(is_rotor)
    def _():
        trace(NODES - 1, LANES - SLAB)

    @pl.when(jnp.logical_not(is_rotor))
    def _():
        trace(0, 0)


def pack_kernel(state, flow_in, offset_in, frac_in, *refs):
    x, first, other, flow, frac = refs[:5]
    turns, (offset, *arrivals) = refs[5:9], refs[9:]
    pairs = [(flow_in, flow), (offset_in, offset), (frac_in, frac)]
    pairs.append((state, x))
    copies = [pltpu.make_async_copy(*pair, sem) for pair, sem in zip(pairs, arrivals)]
    for copy in copies:
        copy.start()
    for copy in copies[:3]:
        copy.wait()
    for section in range(2):
        turns[2 * section][0] = lax.shift_right_logical(offset[section], 3)
        turns[2 * section + 1][0] = offset[section] & (LOW - 1)
    copies[3].wait()
    pack(x, first, other)


def stay_kernel(source, target, done):
    copy = pltpu.make_async_copy(source, target, done)
    copy.start()
    copy.wait()


def mortar_kernel(frac, own, beyond, out, *, section):
    is_rotor = lax.axis_index("blk") == 0
    index = frac[section]
    whole = lax.shift_right_logical(index, 2)
    part = (index & (FRACS - 1)).astype(jnp.float32) * (1.0 / FRACS)
    begin = jnp.where(is_rotor, EA - 1 - whole, whole)
    scaled = by_row((POINTS + 1.0) / 2.0)
    for_stator = scaled - part
    for_rotor = scaled + part
    at = jnp.where(is_rotor, for_stator, for_rotor)
    upper = jnp.where(
        is_rotor, (scaled > part).astype(jnp.int32), (for_rotor >= 1.0).astype(jnp.int32)
    )
    step = jnp.where(is_rotor, 1 - upper, -upper).astype(jnp.float32)
    is_upper = upper == 1
    local = (at + step) * 2.0 - 1.0
    weights = []
    for s in range(NODES):
        weight = jnp.ones((NODES, LANES), jnp.float32)
        for j in range(NODES):
            if j != s:
                weight = weight * ((local - float(POINTS[j])) * float(1.0 / (POINTS[s] - POINTS[j])))
        weights.append(weight)
    slot = iota(1) & (EA - 1)

    def window(lead, trail, begin):
        return jnp.where(
            slot + begin < EA,
            pltpu.roll(lead, (LANES - begin) & (LANES - 1), 1),
            pltpu.roll(trail, (LANES + EA - begin) & (LANES - 1), 1),
        )

    for p in range(TRACE_TILES):
        mine = own[tile(FACE_TILES + p)]
        theirs = beyond[tile(FACE_TILES + p)]
        lead = jnp.where(is_rotor, theirs, mine)
        trail = jnp.where(is_rotor, mine, theirs)
        low = window(lead, trail, begin)
        high = window(lead, trail, begin + 1)
        total = None
        for s in range(NODES):
            pick = jnp.where(
                is_upper,
                jnp.broadcast_to(high[s : s + 1, :], (NODES, LANES)),
                jnp.broadcast_to(low[s : s + 1, :], (NODES, LANES)),
            )
            total = weights[s] * pick if total is None else total + weights[s] * pick
        out[tile(p)] = total


def close_kernel(flow, acc, x, first, other, first_own, other_own, plus, *refs, second):
    if second:
        target, out, arrived, inner, bottom_sent, top_sent, arrival = refs
        messages = ()
    else:
        out, *messages, arrived, arrival = refs
    fetch = pltpu.make_async_copy(plus, arrived, arrival)
    fetch.start()
    gain = TIME_STEP * (0.5 if second else 1.0)
    row = lax.axis_index("blk")
    is_rotor = row == 0
    speed = [flow[row, at] for at in range(3)]
    sound = flow[row, 3]
    far_speed, far_sound = flow[1 - row, 2], flow[1 - row, 3]
    wide = [spread(flow, at + 1) for at in range(3)]
    lane = iota(1)
    slot = lane & (EA - 1)
    layer = lax.shift_right_logical(lane, 5)
    factor = gain * LIFT * azimuth_scale()
    lower, upper = [], []
    for v in range(VARS):
        one = first[tile(v)] - other_own[tile(v)]
        two = other[tile(v)] - first_own[tile(v)]
        lower.append(jnp.where(is_rotor, one, two))
        upper.append(jnp.where(is_rotor, two, one))
    lower = jump_rates(lower, 1, -1.0, speed[0], sound, wide[0], factor)
    upper = jump_rates(upper, 1, 1.0, speed[0], sound, wide[0], factor)

    def at_layer(i, carry):
        for v in range(VARS):
            out[v, i] = acc[v, i]
            west = pltpu.roll(lower[v], (LANES - i) & (LANES - 1), 1)
            east = pltpu.roll(upper[v], EA - 1 - i, 1)
            out[v, i, :, 0, :] = acc[v, i, :, 0, :] + jnp.where(slot == 0, west, 0.0)
            last = acc[v, i, :, NODES - 1, :] + jnp.where(slot == EA - 1, east, 0.0)
            out[v, i, :, NODES - 1, :] = last
        return carry

    lax.fori_loop(1, NODES - 1, at_layer, 0)
    if second:
        inside = (slice(None), slice(1, NODES - 1))
        send = pltpu.make_async_copy(out.at[inside], target.at[inside], inner)
        send.start()
    lax.fori_loop(0, 2, lambda side, carry: at_layer(side * (NODES - 1), carry), 0)
    fetch.wait()

    def interface(plane, start, normal):
        scale = -gain * LIFT * 2.0
        mine = scale * 0.5 * (wide[2] - normal * speed[2])
        theirs = scale * 0.5 * (normal * far_speed - wide[2])
        cross_mine = -scale * 0.5 * normal * sound
        cross_theirs = scale * 0.5 * normal * far_sound
        for b in range(NODES):
            inside = [x[v, plane, b] for v in range(VARS)]
            outside = []
            for v in range(VARS):
                p, o = divmod(v * NODES + b, EZ)
                outside.append(turned(arrived[tile(p)], start - SLAB * o))
            for v in range(VARS):
                term = mine * inside[v] + theirs * outside[v]
                if v == 0 or v == 3:
                    term = term + (cross_mine * inside[3 - v] + cross_theirs * outside[3 - v])
                out[v, plane, b] = out[v, plane, b] + jnp.where(layer == start // SLAB, term, 0.0)

    @pl.when(is_rotor)
    def _():
        interface(NODES - 1, LANES - SLAB, 1.0)

    @pl.when(jnp.logical_not(is_rotor))
    def _():
        interface(0, 0, -1.0)

    if messages:
        pack(out, *messages)
    if second:
        bottom = pltpu.make_async_copy(out.at[:, 0], target.at[:, 0], bottom_sent)
        top = pltpu.make_async_copy(out.at[:, NODES - 1], target.at[:, NODES - 1], top_sent)
        bottom.start()
        top.start()
        send.wait()
        bottom.wait()
        top.wait()


VMEM = pl.BlockSpec(memory_space=pltpu.VMEM)
SMEM = pl.BlockSpec(memory_space=pltpu.SMEM)
HBM = pl.BlockSpec(memory_space=pltpu.HBM)
BLOCK = (VARS, NODES, NODES, NODES, LANES)
FIRST = (80, LANES)
OTHER = (32, LANES)
TRACE = (TRACE_TILES * NODES, LANES)


def call(body, scalars, arrays, shapes, name, flops=1000, **more):
    arrays = [pltpu.with_memory_space_constraint(array, pltpu.VMEM) for array in arrays]
    outs = [pltpu.VMEM(shape, jnp.float32) for shape in shapes] + more.pop("more_outs", [])
    specs = [VMEM for _ in shapes] + more.pop("more_specs", [])
    others = [
        pltpu.with_memory_space_constraint(array, pltpu.HBM) for array in more.pop("others", [])
    ]
    results = pl.pallas_call(
        body,
        in_specs=[SMEM] * len(scalars) + [VMEM] * len(arrays) + [HBM] * len(others),
        out_specs=tuple(specs),
        out_shape=tuple(outs),
        cost_estimate=pl.CostEstimate(flops=flops, transcendentals=0, bytes_accessed=10**6),
        compiler_params=pltpu.CompilerParams(vmem_limit_bytes=16 * 2**20),
        name=name,
        **more,
    )(*scalars, *arrays, *others)
    return results if len(results) > 1 else results[0]


def stay(array):
    return pl.pallas_call(
        stay_kernel,
        in_specs=[HBM],
        out_specs=HBM,
        out_shape=jax.ShapeDtypeStruct(TRACE, jnp.float32),
        scratch_shapes=[pltpu.SemaphoreType.DMA(())],
        name="stay",
    )(array)


def rotated(message, high, low, count):
    def far(turn):
        shift = LOW * turn
        pairs = [(i, count + (i + shift) % count) for i in range(count)]
        pairs += [(count + (i + shift) % count, i) for i in range(count)]
        return lambda array: lax.ppermute(array, AXES, pairs)

    def near(turn):
        if turn == 0:
            return stay
        pairs = [(i, (i - turn) % count) for i in range(count)]
        pairs += [(count + i, count + (i + turn) % count) for i in range(count)]
        return lambda array: lax.ppermute(array, AXES, pairs)

    message = lax.switch(high, [far(at) for at in range(count // LOW)], message)
    return lax.switch(low, [near(at) for at in range(LOW)], message)


def per_device(state, mean_flow, sector_offset, frac_index):
    count = lax.axis_size("sector")
    ahead = [(i, (i + 1) % count) for i in range(count)]
    ahead += [(count + (i + 1) % count, count + i) for i in range(count)]
    back = [(j, i) for i, j in ahead]
    start, first, other, flow, frac, *turns = call(
        pack_kernel,
        [],
        [],
        (BLOCK, FIRST, OTHER),
        "pack",
        others=[state, mean_flow, sector_offset, frac_index],
        more_outs=[pltpu.SMEM((2, 4), jnp.float32), pltpu.SMEM((2,), jnp.int32)]
        + [pltpu.SMEM((1,), jnp.int32)] * 4,
        more_specs=[SMEM] * 6,
        scratch_shapes=[pltpu.SMEM((2,), jnp.int32)] + [pltpu.SemaphoreType.DMA(())] * 4,
    )
    current = start
    flow = pltpu.with_memory_space_constraint(flow, pltpu.SMEM)
    frac = pltpu.with_memory_space_constraint(frac, pltpu.SMEM)
    for section in range(2):
        second = section == 1
        first_in = lax.ppermute(first, AXES, ahead)
        other_in = lax.ppermute(other, AXES, back)
        partial = call(
            functools.partial(volume_kernel, second=second),
            [flow],
            [start, current] if second else [current],
            (BLOCK,),
            "volume",
            flops=10**8,
        )
        message = call(
            functools.partial(mortar_kernel, section=section),
            [frac],
            [first, first_in],
            (TRACE,),
            "mortar",
        )
        high, low = turns[2 * section].reshape(()), turns[2 * section + 1].reshape(())
        plus = rotated(message, high, low, count)
        scratch = [pltpu.VMEM(TRACE, jnp.float32)]
        if second:
            scratch = [pltpu.VMEM(BLOCK, jnp.float32)] + scratch
            semaphores = [pltpu.SemaphoreType.DMA(())] * 4
            more = {
                "more_outs": [jax.ShapeDtypeStruct(BLOCK, jnp.float32)],
                "more_specs": [HBM],
            }
        else:
            semaphores = [pltpu.SemaphoreType.DMA(())]
            more = {}
        results = call(
            functools.partial(close_kernel, second=second),
            [flow],
            [partial, current, first_in, other_in, first, other],
            () if second else (BLOCK, FIRST, OTHER),
            "close",
            others=[plus],
            scratch_shapes=scratch + semaphores,
            **more,
        )
        if not second:
            current, first, other = results
    return results


def solution(mesh):
    in_specs = (P(None, None, None, None, ("blk", "sector")), P(), P(), P())
    out_specs = P(None, None, None, None, ("blk", "sector"))
    return jax.shard_map(
        per_device, mesh=mesh, in_specs=in_specs, out_specs=out_specs, check_vma=False
    )
```
